256 devices in a mesh: row: 16 (over x, y), col: 16 (over z, core).
Axes of the slice: x: 4, y: 4, z: 8, core: 2. Of those that a mesh axis runs over, the one named last changes fastest.
Arguments:
- inverse_factor: bfloat16 [8192, 8192], P('row', 'col'), may hold values from -1 to 2, as said below
- alpha_vector: float32 [8192], replicated, may hold values from -2 to 2
Outputs:
- weight_matrix: float32 [8192, 8192], P(('row', 'col'))
The draws below stay inside these ranges and needn't reach their ends.
Inputs may be any that keep to these rules, and one draw needn't show every extreme that they name: `inverse_factor`: lower triangular: every entry above the diagonal is zero; diagonal entries lie between 1 and 2.
All inputs are finite; a program needn't handle non-finite values.
Results may differ from the reference program's by a relative error of at most 0.0003.
Values may be sent and summed in bfloat16 or wider, within the bound.
A program may use at most 64 MiB of HBM per device.

```python
import jax
import jax.numpy as jnp

N = 8192


def draw_inverse_factor(key, part):
    first = jax.random.fold_in(key, 11)
    second = jax.random.fold_in(key, 23)
    spread = jnp.clip(jax.random.normal(first, (N, N), jnp.float32), -6.0, 6.0)
    diagonal = jnp.exp(jax.random.uniform(second, (N,), jnp.float32, 0.0, 0.6931472))
    lower = jnp.tril(spread * (2.0 / jnp.sqrt(jnp.float32(N))), -1)
    return (lower + jnp.diag(diagonal)).astype(jnp.bfloat16)


def bell_draw(key, dims, scale, bound, held_as=jnp.bfloat16):
    drawn = jax.random.normal(key, dims, jnp.float32) * scale
    return jnp.minimum(jnp.maximum(drawn, -bound), bound).astype(held_as)


def setup_inputs(seed: int = 0) -> dict:
    key_list = jax.random.split(jax.random.key(seed), 3)
    return {
        "inverse_factor": draw_inverse_factor(jax.random.fold_in(key_list[2], 71), 0),
        "alpha_vector": bell_draw(key_list[1], (N,), 0.3, 2.0, jnp.float32),
    }


def reference(inverse_factor, alpha_vector):
    gram = jnp.dot(inverse_factor.T, inverse_factor, preferred_element_type=jnp.float32)
    return gram - alpha_vector[:, None] * alpha_vector[None, :]
```

```python
import functools

import jax
import jax.numpy as jnp
from jax import lax
from jax.experimental import pallas as pl
from jax.experimental.pallas import tpu as pltpu
from jax.sharding import PartitionSpec as P

MESH = pl.DeviceIdType.MESH
D = 16


def div(a, b):
    return lax.div(a, jnp.int32(b))


def rem(a, b):
    return lax.rem(a, jnp.int32(b))


def fold(c):
    return c + div(c, 8) * (15 - 2 * c)


def kernel(B, a_ref, out_ref, at, sbuf, jbuf, acc, s_send, s_recv, own_send, j_first, j_send, j_extra, j_recv, o_send, o_recv):
    T, H, R = B // D, B // 2, (B // D) * 17
    half = R // 2
    row, col = lax.axis_index("row"), lax.axis_index("col")
    x, y, core = div(row, 4), rem(row, 4), rem(col, 2)
    sign = 1 - 2 * core
    m = fold(row)

    def remote(src, dst, send, recv, r, c):
        return pltpu.make_async_remote_copy(
            src_ref=src, dst_ref=dst, send_sem=send, recv_sem=recv, device_id=(r, c), device_id_type=MESH
        )

    mirror = 15 - row
    upper = div(col, 8)
    mc = fold(col)
    j_col = row + upper * (15 - 2 * row)
    j_row = (mc, 15 - mc)
    j_slot = row + 16 * upper
    full = row >= col
    j_from = ((col, m), (15 - col, 15 - m))

    barrier = pltpu.get_barrier_semaphore()

    def greet(r, c):
        pl.semaphore_signal(barrier, inc=1, device_id=(r, c), device_id_type=MESH)

    @pl.loop(1, D)
    def _(k):
        greet(row, rem(col + k, D))
        greet(rem(row + k, D), col)

    @pl.loop(0, D)
    def _(k):
        greet(mirror, rem(col + k, D))

    for k, (r, c) in enumerate(j_from):
        valid = (col >= m) if k == 0 else (col <= m)

        @pl.when(jnp.logical_and(valid, jnp.logical_or(r != row, c != col)))
        def _(r=r, c=c):
            greet(r, c)

    at[...] = jnp.transpose(a_ref[...])
    n_full = div(row + 16 - col, 16)
    n_self = n_full * div(col + 16 - row, 16) * (1 - upper)
    pl.semaphore_wait(barrier, 46 + 2 * n_full - n_self)

    def first(h):
        return remote(
            a_ref.at[:, pl.ds(h * H, H)], jbuf.at[j_slot], j_first.at[h], j_recv.at[j_slot], j_row[h], j_col
        )

    for h in range(2):
        to_self = jnp.logical_and(j_row[h] == row, j_col == col)

        @pl.when(jnp.logical_and(full, jnp.logical_not(to_self)))
        def _(h=h):
            first(h).start()

        @pl.when(jnp.logical_and(full, to_self))
        def _(h=h):
            pltpu.make_async_copy(a_ref.at[:, pl.ds(h * H, H)], jbuf.at[j_slot], j_recv.at[j_slot]).start()

    piece = pl.multiple_of(T * col, T)
    low = sbuf.at[row, pl.ds(piece, T), :]
    high = sbuf.at[mirror, pl.ds(pl.multiple_of(T * (16 - row), T) + piece, T), :]

    @pl.when(full)
    def _():
        @pl.loop(1, D)
        def _(k):
            i = rem(col + k, D)
            src = at.at[pl.ds(pl.multiple_of(T * i, T), T), pl.ds(0, H)]
            remote(src, low, own_send, s_recv.at[0, row], row, i).start()

        pltpu.make_async_copy(at.at[pl.ds(piece, T), pl.ds(0, H)], low, s_recv.at[0, row]).start()

        @pl.loop(0, D)
        def _(k):
            i = rem(col + k, D)
            src = at.at[pl.ds(pl.multiple_of(T * i, T), T), pl.ds(H, H)]
            remote(src, high, own_send, s_recv.at[0, mirror], mirror, i).start()

    s_sent = []

    def s_row(dx, dy, sg):
        return rem(x - sg * dx + 8, 4) * 4 + rem(y - sg * dy + 8, 4)

    def s_copy(h, slot, tx, ty, sg):
        part = sbuf.at[slot, pl.ds(h * half, half), :]
        k = len(s_sent)
        c = remote(part, part, s_send.at[k], s_recv.at[h, slot], s_row(-tx, -ty, sg), col)
        c.start()
        s_sent.append(c)

    def s_wait(h, slot):
        part = sbuf.at[slot, pl.ds(h * half, half), :]
        pltpu.make_async_copy(part, part, s_recv.at[h, slot]).wait()

    def s_step(h, d1, d2):
        sg = sign if h == 0 else -sign
        at_ = (lambda p, s: (p, s)) if h == 0 else (lambda p, s: (s, p))
        slot = s_row(*at_(d1, d2), sg)
        if (d1, d2) != (0, 0):
            s_wait(h, slot)
        if d2 == 0:
            if d1 in (0, 1):
                s_copy(h, slot, *at_(1, 0), sg)
            if d1 == 0:
                s_copy(h, slot, *at_(-1, 0), sg)
            s_copy(h, slot, *at_(0, 1), sg)
            s_copy(h, slot, *at_(0, -1), sg)
        elif d2 == 1:
            s_copy(h, slot, *at_(0, 1), sg)

    j_sent, j_extras = [], []

    def j_main(t):
        ge = div(t + 16 - m, 16)
        return t * ge + (31 - t) * (1 - ge)

    def j_wait(slot):
        pltpu.make_async_copy(jbuf.at[slot], jbuf.at[slot], j_recv.at[slot]).wait()

    other = col + sign

    def j_step(t, targets):
        slot = j_main(t)
        j_wait(slot)
        base = len(j_sent)
        for n, c in enumerate(targets):
            cp = remote(jbuf.at[slot], jbuf.at[slot], j_send.at[base + n], j_recv.at[slot], row, c)
            cp.start()
            j_sent.append(cp)
        xs = 31 - m

        def extra(n, c):
            return remote(jbuf.at[xs], jbuf.at[xs], j_extra.at[base + n], j_recv.at[xs], row, c)

        @pl.when(t == m)
        def _():
            j_wait(xs)
            for n, c in enumerate(targets):
                extra(n, c).start()

        j_extras.append((t, [functools.partial(extra, n, c) for n, c in enumerate(targets)]))

    def z_at(d):
        return rem(col + 2 * sign * d + 32, D)

    s_wait_all = pltpu.make_async_copy(sbuf.at[row], sbuf.at[row], s_recv.at[0, row])
    s_wait_all.wait()
    for h in range(2):
        s_step(h, 0, 0)
    j_step(col, (z_at(1), z_at(-1), other))
    s_order = [
        [(1, 0), (-1, 0), (0, 1)],
        [(2, 0), (1, 1), (-1, 1)],
        [(2, 1)],
        [],
    ]
    for level in range(4):
        for d1, d2 in s_order[level]:
            for h in range(2):
                s_step(h, d1, d2)
        d = level + 1
        j_step(z_at(-d), ((z_at(1),) if d < 4 else ()) + (other,))
        if d < 4:
            j_step(z_at(d), ((z_at(-1),) if d < 3 else ()) + (other,))
    for d1, d2 in [(0, -1), (0, 2), (1, -1), (-1, -1), (1, 2), (-1, 2), (2, -1), (2, 2)]:
        for h in range(2):
            s_step(h, d1, d2)
    for d in range(8):
        j_step(rem(other + 2 * d, D), ())

    acc[...] = jnp.zeros_like(acc)
    for q in reversed(range(D)):
        n = T * (q + 1)
        for h in range(2):

            @pl.when((q >= m) if h == 0 else (q >= 15 - m))
            def _(q=q, n=n, h=h):
                slot = q + 16 * h
                acc[h, 0:n, :] += jnp.dot(
                    sbuf[q, 0:n, :], jbuf[slot, 0:H, :], preferred_element_type=jnp.float32
                ) + jnp.dot(
                    sbuf[15 - q, R - n : R, :], jbuf[slot, H:B, :], preferred_element_type=jnp.float32
                )

    shift = H * div(row, 8)
    starts = (pl.multiple_of(m * B + shift, H), pl.multiple_of((15 - m) * B + shift, H))
    for h in range(2):
        pltpu.make_async_copy(
            acc.at[h, pl.ds(pl.multiple_of(T * row, T), T), :], out_ref.at[:, pl.ds(starts[h], H)], o_recv
        ).start()

    @pl.loop(1, D)
    def _(k):
        r = rem(row + k, D)
        for h in range(2):
            remote(
                acc.at[h, pl.ds(pl.multiple_of(T * r, T), T), :], out_ref.at[:, pl.ds(starts[h], H)], o_send, o_recv, r, col
            ).start()

    for h in range(2):
        to_self = jnp.logical_and(j_row[h] == row, j_col == col)

        @pl.when(jnp.logical_and(full, jnp.logical_not(to_self)))
        def _(h=h):
            first(h).wait_send()

    @pl.when(full)
    def _():
        sent = at.at[pl.ds(0, T * 15 + T // 2), :]
        pltpu.make_async_copy(sent, sent, own_send).wait()

    for c in s_sent:
        c.wait_send()
    for c in j_sent:
        c.wait_send()
    for t, extras in j_extras:
        if extras:

            @pl.when(t == m)
            def _(extras=extras):
                for e in extras:
                    e().wait_send()

    done = acc.at[:, pl.ds(0, B - T), :]
    pltpu.make_async_copy(done, done, o_send).wait()
    pltpu.make_async_copy(out_ref, out_ref, o_recv).wait()


def solution(mesh):
    def body(a, alpha):
        B = a.shape[0]
        N = B * D
        T, R = B // D, (B // D) * 17
        g = pl.pallas_call(
            functools.partial(kernel, B),
            out_shape=jax.ShapeDtypeStruct((T, N), jnp.float32),
            in_specs=[pl.BlockSpec(memory_space=pltpu.VMEM)],
            out_specs=pl.BlockSpec(memory_space=pltpu.VMEM),
            scratch_shapes=[
                pltpu.VMEM((B, B), jnp.bfloat16),
                pltpu.VMEM((D, R, B // 2), jnp.bfloat16),
                pltpu.VMEM((2 * D, B, B // 2), jnp.bfloat16),
                pltpu.VMEM((2, B, B // 2), jnp.float32),
                pltpu.SemaphoreType.DMA((30,)),
                pltpu.SemaphoreType.DMA((2, D)),
                pltpu.SemaphoreType.DMA,
                pltpu.SemaphoreType.DMA((2,)),
                pltpu.SemaphoreType.DMA((16,)),
                pltpu.SemaphoreType.DMA((16,)),
                pltpu.SemaphoreType.DMA((2 * D,)),
                pltpu.SemaphoreType.DMA,
                pltpu.SemaphoreType.DMA,
            ],
            compiler_params=pltpu.CompilerParams(
                collective_id=0, has_side_effects=True, vmem_limit_bytes=40 * 1024 * 1024
            ),
        )(a)
        start = (lax.axis_index("row") * D + lax.axis_index("col")) * T
        mine = lax.dynamic_slice(alpha, (start,), (T,))
        return g - mine[:, None] * alpha[None, :]

    return jax.shard_map(
        body, mesh=mesh, in_specs=(P("row", "col"), P(None)), out_specs=P(("row", "col"), None), check_vma=False
    )
```

```python
import functools

import jax
import jax.numpy as jnp
from jax import lax
from jax.experimental import pallas as pl
from jax.experimental.pallas import tpu as pltpu
from jax.sharding import PartitionSpec as P

MESH = pl.DeviceIdType.MESH
D = 16


def div(a, b):
    return lax.div(a, jnp.int32(b))


def rem(a, b):
    return lax.rem(a, jnp.int32(b))


def kernel(st, B, a_ref, out_ref, at, sbuf, jbuf, acc, swp, got, s_send, s_recv, own_send, x_send, x_recv, j_send, j_recv, o_send, o_recv):
    T, H, R = B // D, B // 2, (B // D) * 17
    Q, half = T // 2, R // 2
    row, col = lax.axis_index("row"), lax.axis_index("col")
    x, y, core = div(row, 4), rem(row, 4), rem(col, 2)
    sign = 1 - 2 * core
    mirror = 15 - row
    full = row >= col

    def rows(start, n):
        return pl.ds(pl.multiple_of(start, Q), n)

    def remote(src, dst, send, recv, r, c):
        return pltpu.make_async_remote_copy(
            src_ref=src, dst_ref=dst, send_sem=send, recv_sem=recv, device_id=(r, c), device_id_type=MESH
        )

    def wait_bytes(ref, sem):
        pltpu.make_async_copy(ref, ref, sem).wait()

    barrier = pltpu.get_barrier_semaphore()

    def greet(r, c):
        pl.semaphore_signal(barrier, inc=1, device_id=(r, c), device_id_type=MESH)

    @pl.loop(0, D)
    def _(k):
        greet(mirror, rem(col + k, D))

    @pl.loop(1, D)
    def _(k):
        greet(row, rem(col + k, D))
        greet(rem(row + k, D), col)

    at[...] = jnp.transpose(a_ref[...])
    pl.semaphore_wait(barrier, 46)

    if "f" in st:
        piece = T * col
        low = sbuf.at[row, rows(piece, T), :]
        high = sbuf.at[mirror, rows(T * (16 - row) + piece, T), :]

        @pl.when(full)
        def _():
            pltpu.make_async_copy(at.at[rows(piece, T), pl.ds(0, H)], low, s_recv.at[0, row]).start()

            @pl.loop(1, D)
            def _(k):
                i = rem(col + k, D)
                remote(at.at[rows(T * i, T), pl.ds(0, H)], low, own_send, s_recv.at[0, row], row, i).start()

            @pl.loop(0, D)
            def _(k):
                i = rem(col + k, D)
                remote(at.at[rows(T * i, T), pl.ds(H, H)], high, own_send, s_recv.at[0, mirror], mirror, i).start()

        wait_bytes(sbuf.at[row], s_recv.at[0, row])

    if "x" in st:
        here = row * T

        def pair(p):
            gx = div(row + 16 - p, 16)
            gy = div(row + 1 + p, 16)
            base = T * (row + 1)
            first = gx * (T * p) + (1 - gx) * (base + T * (15 - p) + Q)
            second = gy * (T * (15 - p) + Q) + (1 - gy) * (base + T * p)
            return first, second

        for n, start in enumerate(pair(row)):
            pltpu.make_async_copy(sbuf.at[row, rows(start, Q), :], jbuf.at[col, rows(here + Q * n, Q), :], x_recv).start()
        pltpu.make_async_copy(sbuf.at[row, pl.ds(B + Q, Q), :], jbuf.at[col, pl.ds(B, Q), :], x_recv).start()
        remote(sbuf.at[row, pl.ds(B, Q), :], jbuf.at[col, pl.ds(B + Q, Q), :], x_send, x_recv, mirror, col).start()

        @pl.loop(1, D)
        def _(k):
            p = rem(row + k, D)
            for n, start in enumerate(pair(p)):
                remote(sbuf.at[row, rows(start, Q), :], jbuf.at[col, rows(here + Q * n, Q), :], x_send, x_recv, p, col).start()

    s_sent = []

    def s_row(dx, dy, sg):
        return rem(x - sg * dx + 8, 4) * 4 + rem(y - sg * dy + 8, 4)

    def s_copy(h, slot, tx, ty, sg):
        part = sbuf.at[slot, pl.ds(h * half, half), :]
        c = remote(part, part, s_send.at[len(s_sent)], s_recv.at[h, slot], s_row(-tx, -ty, sg), col)
        c.start()
        s_sent.append(c)

    def s_step(h, d1, d2):
        if "s" not in st:
            return
        sg = sign if h == 0 else -sign
        turn = (lambda p, s: (p, s)) if h == 0 else (lambda p, s: (s, p))
        slot = s_row(*turn(d1, d2), sg)
        if (d1, d2) != (0, 0):
            wait_bytes(sbuf.at[slot, pl.ds(h * half, half), :], s_recv.at[h, slot])
        if d2 == 0:
            if d1 in (0, 1):
                s_copy(h, slot, *turn(1, 0), sg)
            if d1 == 0:
                s_copy(h, slot, *turn(-1, 0), sg)
            s_copy(h, slot, *turn(0, 1), sg)
            s_copy(h, slot, *turn(0, -1), sg)
        elif d2 == 1:
            s_copy(h, slot, *turn(0, 1), sg)

    j_sent = []
    other = col + sign

    def z_at(d):
        return rem(col + 2 * sign * d + 32, D)

    def j_step(t, targets, own=False):
        if "j" not in st:
            return
        if not own:
            wait_bytes(jbuf.at[t], j_recv.at[t])
        for c in targets:
            cp = remote(jbuf.at[t], jbuf.at[t], j_send.at[len(j_sent)], j_recv.at[t], row, c)
            cp.start()
            j_sent.append(cp)

    for h in range(2):
        s_step(h, 0, 0)
    if "x" in st:
        wait_bytes(jbuf.at[col], x_recv)
    j_step(col, (z_at(1), z_at(-1), other), True)
    s_order = [
        [(1, 0), (-1, 0), (0, 1)],
        [(2, 0), (1, 1), (-1, 1)],
        [(2, 1)],
        [],
    ]
    for level in range(4):
        for d1, d2 in s_order[level]:
            for h in range(2):
                s_step(h, d1, d2)
        d = level + 1
        j_step(z_at(-d), ((z_at(1),) if d < 4 else ()) + (other,))
        if d < 4:
            j_step(z_at(d), ((z_at(-1),) if d < 3 else ()) + (other,))
    for d1, d2 in [(0, -1), (0, 2), (1, -1), (-1, -1), (1, 2), (-1, 2), (2, -1), (2, 2)]:
        for h in range(2):
            s_step(h, d1, d2)
    for d in range(8):
        j_step(rem(other + 2 * d, D), ())

    if "c" in st:
        early = rem(lax.broadcasted_iota(jnp.int32, (1, B), 1), T) < Q
        acc[...] = jnp.zeros_like(acc)
        swp[...] = jnp.zeros_like(swp)
        other_row = 15 - row
        for s in range(D):

            def add(ref, lhs, n, start, first, second, s=s):
                right = jbuf[:, start : start + T, :].reshape(B, H)
                prod = lax.dot_general(lhs, right, (((1,), (1,)), ((), ())), preferred_element_type=jnp.float32)
                keep = jnp.logical_or(jnp.logical_and(early, first), jnp.logical_and(jnp.logical_not(early), second))
                ref[0:n, :] += jnp.where(keep, prod, 0.0)

            n = T * (s + 1)

            @pl.when(jnp.logical_or(s >= row, s >= other_row))
            def _(s=s, n=n, add=add):
                add(acc, sbuf[s, 0:n, :], n, T * s, s >= row, s >= other_row)

            k = R - n

            @pl.when(jnp.logical_or(s < row, s < other_row))
            def _(s=s, n=n, k=k, add=add):
                add(swp, sbuf[s, n:R, :], k, T * s, s < row, s < other_row)

            @pl.when(jnp.logical_or(s == row, s == other_row))
            def _(s=s, n=n, k=k, add=add):
                add(swp, sbuf[s, n:R, :], k, B, s == row, s == other_row)

        acc[...] += jnp.where(early, pltpu.roll(swp[...], B - Q, 1), pltpu.roll(swp[...], Q, 1))

    if "o" in st:
        pltpu.make_async_copy(acc.at[rows(T * row, T), :], got.at[row], o_recv).start()

        @pl.loop(1, D)
        def _(k):
            r = rem(row + k, D)
            remote(acc.at[rows(T * r, T), :], got.at[row], o_send, o_recv, r, col).start()

    if "f" in st:

        @pl.when(full)
        def _():
            wait_bytes(at.at[pl.ds(0, T * 15 + T // 2), :], own_send)

    if "x" in st:
        wait_bytes(sbuf.at[row, pl.ds(0, B - Q), :], x_send)
    for c in s_sent + j_sent:
        c.wait_send()
    if "o" in st:
        wait_bytes(acc.at[pl.ds(0, B - T), :], o_send)
        wait_bytes(got, o_recv)
    early = rem(lax.broadcasted_iota(jnp.int32, (1, B), 1), T) < Q
    for b in range(D):
        out_ref[:, B * b : B * (b + 1)] = jnp.where(early, got[b], got[15 - b])


def solution(mesh, st="fxsjco"):
    def body(a, alpha):
        B = a.shape[0]
        T, R = B // D, (B // D) * 17
        g = pl.pallas_call(
            functools.partial(kernel, st, B),
            out_shape=jax.ShapeDtypeStruct((T, B * D), jnp.float32),
            in_specs=[pl.BlockSpec(memory_space=pltpu.VMEM)],
            out_specs=pl.BlockSpec(memory_space=pltpu.VMEM),
            scratch_shapes=[
                pltpu.VMEM((B, B), jnp.bfloat16),
                pltpu.VMEM((D, R, B // 2), jnp.bfloat16),
                pltpu.VMEM((D, R, B // 2), jnp.bfloat16),
                pltpu.VMEM((B, B), jnp.float32),
                pltpu.VMEM((B, B), jnp.float32),
                pltpu.VMEM((D, T, B), jnp.float32),
                pltpu.SemaphoreType.DMA((30,)),
                pltpu.SemaphoreType.DMA((2, D)),
                pltpu.SemaphoreType.DMA,
                pltpu.SemaphoreType.DMA,
                pltpu.SemaphoreType.DMA,
                pltpu.SemaphoreType.DMA((15,)),
                pltpu.SemaphoreType.DMA((D,)),
                pltpu.SemaphoreType.DMA,
                pltpu.SemaphoreType.DMA,
            ],
            compiler_params=pltpu.CompilerParams(
                collective_id=0, has_side_effects=True, vmem_limit_bytes=40 * 1024 * 1024
            ),
        )(a)
        start = (lax.axis_index("row") * D + lax.axis_index("col")) * T
        mine = lax.dynamic_slice(alpha, (start,), (T,))
        return g - mine[:, None] * alpha[None, :]

    return jax.shard_map(
        body, mesh=mesh, in_specs=(P("row", "col"), P(None)), out_specs=P(("row", "col"), None), check_vma=False
    )
```

```python
import functools

import jax
import jax.numpy as jnp
from jax import lax
from jax.experimental import pallas as pl
from jax.experimental.pallas import tpu as pltpu
from jax.sharding import PartitionSpec as P

MESH = pl.DeviceIdType.MESH
D = 16
SUB = 2
VM = 40 * 1024 * 1024


def div(a, b):
    return lax.div(a, jnp.int32(b))


def rem(a, b):
    return lax.rem(a, jnp.int32(b))


def kernel(
    st,
    B,
    a_hbm,
    alpha_ref,
    out_ref,
    a_ref,
    at,
    sbuf,
    jbuf,
    acc,
    got,
    a_sem,
    s_send,
    s_recv,
    own_send,
    x_send,
    x_recv,
    j_send,
    j_recv,
    o_send,
    o_recv,
):
    T, H, R = B // D, B // 2, (B // D) * 17
    Q, half, sub = T // 2, R // 2, R // SUB
    row, col = lax.axis_index("row"), lax.axis_index("col")
    x, y, core = div(row, 4), rem(row, 4), rem(col, 2)
    sign = 1 - 2 * core
    mirror = 15 - row
    full = row >= col

    def rows(start, n):
        return pl.ds(pl.multiple_of(start, Q), n)

    def remote(src, dst, send, recv, r, c):
        return pltpu.make_async_remote_copy(
            src_ref=src, dst_ref=dst, send_sem=send, recv_sem=recv, device_id=(r, c), device_id_type=MESH
        )

    def wait_bytes(ref, sem):
        pltpu.make_async_copy(ref, ref, sem).wait()

    barrier = pltpu.get_barrier_semaphore()

    def greet(r, c):
        pl.semaphore_signal(barrier, inc=1, device_id=(r, c), device_id_type=MESH)

    load = pltpu.make_async_copy(a_hbm, a_ref, a_sem)
    load.start()

    @pl.loop(0, D)
    def _(k):
        greet(mirror, rem(col + k, D))

    @pl.loop(1, D)
    def _(k):
        greet(row, rem(col + k, D))
        greet(rem(row + k, D), col)

    load.wait()
    at[...] = jnp.transpose(a_ref[...])
    pl.semaphore_wait(barrier, 46)

    def far_first(k):
        return rem(col + 24 + (1 - 2 * rem(k, 2)) * div(k + 1, 2), D)

    if "f" in st:
        piece = T * col
        low = sbuf.at[row, rows(piece, T), :]
        high = sbuf.at[mirror, rows(T * (16 - row) + piece, T), :]

        @pl.when(full)
        def _():
            @pl.loop(0, D)
            def _(k):
                i = far_first(k)
                remote(at.at[rows(T * i, T), pl.ds(H, H)], high, own_send, s_recv.at[0, mirror], mirror, i).start()

            @pl.loop(0, D - 1)
            def _(k):
                i = far_first(k)
                remote(at.at[rows(T * i, T), pl.ds(0, H)], low, own_send, s_recv.at[0, row], row, i).start()

            pltpu.make_async_copy(at.at[rows(piece, T), pl.ds(0, H)], low, s_recv.at[0, row]).start()

        wait_bytes(sbuf.at[row], s_recv.at[0, row])

    if "x" in st:
        here = row * T

        def pair(p):
            gx = div(row + 16 - p, 16)
            gy = div(row + 1 + p, 16)
            base = T * (row + 1)
            first = gx * (T * p) + (1 - gx) * (base + T * (15 - p) + Q)
            second = gy * (T * (15 - p) + Q) + (1 - gy) * (base + T * p)
            return first, second

        @pl.loop(1, D)
        def _(k):
            p = rem(row + k, D)
            for n, start in enumerate(pair(p)):
                remote(sbuf.at[row, rows(start, Q), :], jbuf.at[col, rows(here + Q * n, Q), :], x_send, x_recv, p, col).start()

        remote(sbuf.at[row, pl.ds(B, Q), :], jbuf.at[col, pl.ds(B + Q, Q), :], x_send, x_recv, mirror, col).start()
        for n, start in enumerate(pair(row)):
            pltpu.make_async_copy(sbuf.at[row, rows(start, Q), :], jbuf.at[col, rows(here + Q * n, Q), :], x_recv).start()
        pltpu.make_async_copy(sbuf.at[row, pl.ds(B + Q, Q), :], jbuf.at[col, pl.ds(B, Q), :], x_recv).start()

    s_sent = []

    def s_row(dx, dy, sg):
        return rem(x - sg * dx + 8, 4) * 4 + rem(y - sg * dy + 8, 4)

    def s_copy(h, slot, tx, ty, sg):
        part = sbuf.at[slot, pl.ds(h * half, half), :]
        c = remote(part, part, s_send.at[len(s_sent)], s_recv.at[h, slot], s_row(-tx, -ty, sg), col)
        c.start()
        s_sent.append(c)

    def s_step(d1, d2):
        if "s" not in st:
            return
        for h in range(2):
            sg = sign if h == 0 else -sign
            turn = (lambda p, s: (p, s)) if h == 0 else (lambda p, s: (s, p))
            slot = s_row(*turn(d1, d2), sg)
            if (d1, d2) != (0, 0):
                wait_bytes(sbuf.at[slot, pl.ds(h * half, half), :], s_recv.at[h, slot])
            if d2 == 0:
                if d1 in (0, 1):
                    s_copy(h, slot, *turn(1, 0), sg)
                if d1 == 0:
                    s_copy(h, slot, *turn(-1, 0), sg)
                s_copy(h, slot, *turn(0, 1), sg)
                s_copy(h, slot, *turn(0, -1), sg)
            elif d2 == 1:
                s_copy(h, slot, *turn(0, 1), sg)

    j_sent = []
    other = col + sign

    def z_at(d):
        return rem(col + 2 * sign * d + 32, D)

    def j_pass(t, u, targets, own=False):
        if "j" not in st:
            return
        part = jbuf.at[t, pl.ds(u * sub, sub), :]
        if not own:
            wait_bytes(part, j_recv.at[t, u])
        for c in targets:
            cp = remote(part, part, j_send.at[len(j_sent)], j_recv.at[t, u], row, c)
            cp.start()
            j_sent.append(cp)

    def j_step(d, u):
        j_pass(z_at(-d), u, ((z_at(1),) if d < 4 else ()) + (other,))
        if d < 4:
            j_pass(z_at(d), u, ((z_at(-1),) if d < 3 else ()) + (other,))

    s_step(0, 0)
    if "x" in st:
        wait_bytes(jbuf.at[col], x_recv)
    for u in range(SUB):
        j_pass(col, u, (z_at(1), z_at(-1)), True)
    for u in range(SUB):
        j_pass(col, u, (other,), True)
    when = [(5.0, s_step, (1, 0)), (5.1, s_step, (-1, 0)), (8.0, s_step, (0, 1)), (9.5, s_step, (2, 0)),
            (12.5, s_step, (1, 1)), (12.6, s_step, (-1, 1)), (17.0, s_step, (2, 1))]
    for d in range(1, 5):
        for u in range(SUB):
            when.append((4 + 5 * d + 6 / SUB * u, j_step, (d, u)))
    for _, step, args in sorted(when, key=lambda e: e[0]):
        step(*args)
    for d1, d2 in [(0, -1), (0, 2), (1, -1), (-1, -1), (1, 2), (-1, 2), (2, -1), (2, 2)]:
        s_step(d1, d2)
    for d in range(8):
        for u in range(SUB):
            j_pass(rem(other + 2 * d, D), u, ())

    def right(start):
        return jbuf[:, start, :].reshape(H, H)

    def times(lhs, rhs):
        return lax.dot_general(lhs, rhs, (((1,), (1,)), ((), ())), preferred_element_type=jnp.float32)

    for g in range(2):
        first_block = mirror if g else row
        if "c" in st:
            acc[g] = jnp.zeros_like(acc[g])
            for q in range(D):
                n = T * (q + 1)

                @pl.when(q >= first_block)
                def _(q=q, n=n, g=g):
                    at_end = 1 - div(q - first_block + 15, 16)
                    start = (1 - at_end) * (T * (15 - q) + Q * (1 - g)) + at_end * (B + Q * (1 - g))
                    acc[g, 0:n, :] += times(sbuf[q, 0:n, :], right(pl.ds(T * q + Q * g, Q))) + times(
                        sbuf[15 - q, R - n : R, :], right(rows(start, Q))
                    )

        if "o" in st:

            @pl.loop(1, D)
            def _(k):
                r = rem(row + k, D)
                remote(acc.at[g, rows(T * r, T), :], got.at[g, row], o_send.at[g], o_recv.at[g], r, col).start()

            pltpu.make_async_copy(acc.at[g, rows(T * row, T), :], got.at[g, row], o_recv.at[g]).start()

    mine = alpha_ref[pl.ds(4 * row + div(col, 4), 1), :]
    mine = pltpu.roll(mine, rem(128 - T * rem(col, 4), 128), 1)
    mine = jnp.transpose(jnp.broadcast_to(mine, (128, 128)))[0:T]

    if "f" in st:

        @pl.when(full)
        def _():
            wait_bytes(at.at[pl.ds(0, T * 15 + T // 2), :], own_send)

    if "x" in st:
        wait_bytes(sbuf.at[row, pl.ds(0, B - Q), :], x_send)
    for c in s_sent + j_sent:
        c.wait_send()
    lane = lax.broadcasted_iota(jnp.int32, (1, 128), 1)
    for g in range(2):
        if "o" in st:
            wait_bytes(got.at[g], o_recv.at[g])
        for b in range(D):
            for k in range(B // 128):
                part = got[g, 15 - b if g else b, :, 128 * (k // 2) : 128 * (k // 2 + 1)]
                start = B * b + 128 * k
                tile = slice(start, start + 128)
                if g == 0:
                    total = -mine * alpha_ref[start // 128 : start // 128 + 1, :]
                else:
                    total = out_ref[:, tile]
                for m in range(4):
                    shift = (Q * m - 64 * (k % 2) + Q * g) % 128
                    moved = pltpu.roll(part, shift, 1) if shift else part
                    total += jnp.where(div(lane, Q) == 2 * m + g, moved, 0.0)
                out_ref[:, tile] = total
    if "o" in st:
        for g in range(2):
            wait_bytes(acc.at[g, pl.ds(0, B - T), :], o_send.at[g])


def solution(mesh, st="fxsjco"):
    def body(a, alpha):
        B = a.shape[0]
        T, H, R = B // D, B // 2, (B // D) * 17
        dma = pltpu.SemaphoreType.DMA
        return pl.pallas_call(
            functools.partial(kernel, st, B),
            out_shape=jax.ShapeDtypeStruct((T, B * D), jnp.float32),
            in_specs=[pl.BlockSpec(memory_space=pltpu.HBM), pl.BlockSpec(memory_space=pltpu.VMEM)],
            out_specs=pl.BlockSpec(memory_space=pltpu.VMEM),
            scratch_shapes=[
                pltpu.VMEM((B, B), jnp.bfloat16),
                pltpu.VMEM((B, B), jnp.bfloat16),
                pltpu.VMEM((D, R, H), jnp.bfloat16),
                pltpu.VMEM((D, R, H), jnp.bfloat16),
                pltpu.VMEM((2, B, H), jnp.float32),
                pltpu.VMEM((2, D, T, H), jnp.float32),
                dma,
                dma((30,)),
                dma((2, D)),
                dma,
                dma,
                dma,
                dma((15 * SUB,)),
                dma((D, SUB)),
                dma((2,)),
                dma((2,)),
            ],
            compiler_params=pltpu.CompilerParams(
                collective_id=0, has_side_effects=True, vmem_limit_bytes=VM
            ),
        )(a, alpha.reshape(B * D // 128, 128))

    return jax.shard_map(
        body, mesh=mesh, in_specs=(P("row", "col"), P(None)), out_specs=P(("row", "col"), None), check_vma=False
    )
```

```python
import functools

import jax
import jax.numpy as jnp
from jax import lax
from jax.experimental import pallas as pl
from jax.experimental.pallas import tpu as pltpu
from jax.sharding import PartitionSpec as P

MESH = pl.DeviceIdType.MESH
D = 16
CUTS = (0, 4, 8, 12, 17)
SUB = len(CUTS) - 1
VM = 40 * 1024 * 1024


def div(a, b):
    return lax.div(a, jnp.int32(b))


def rem(a, b):
    return lax.rem(a, jnp.int32(b))


def fold(c):
    return c + div(c, 8) * (15 - 2 * c)


def kernel(
    st,
    B,
    a_hbm,
    alpha_ref,
    out_ref,
    a_ref,
    at,
    sbuf,
    jbuf,
    acc,
    got,
    a_sem,
    s_send,
    s_recv,
    own_send,
    own_recv,
    x_send,
    x_recv,
    j_send,
    j_recv,
    o_send,
    o_recv,
):
    T, H, R = B // D, B // 2, (B // D) * 17
    Q, half = T // 2, R // 2
    row, col = lax.axis_index("row"), lax.axis_index("col")
    x, y, core = div(row, 4), rem(row, 4), rem(col, 2)
    sign = 1 - 2 * core
    mirror = 15 - row
    full = row >= col
    m = fold(row)

    def rows(start, n):
        return pl.ds(pl.multiple_of(start, Q), n)

    def remote(src, dst, send, recv, r, c):
        return pltpu.make_async_remote_copy(
            src_ref=src, dst_ref=dst, send_sem=send, recv_sem=recv, device_id=(r, c), device_id_type=MESH
        )

    def wait_bytes(ref, sem):
        pltpu.make_async_copy(ref, ref, sem).wait()

    barrier = pltpu.get_barrier_semaphore()

    def greet(r, c):
        pl.semaphore_signal(barrier, inc=1, device_id=(r, c), device_id_type=MESH)

    load = pltpu.make_async_copy(a_hbm, a_ref, a_sem)
    load.start()

    @pl.loop(0, D)
    def _(k):
        greet(mirror, rem(col + k, D))

    @pl.loop(1, D)
    def _(k):
        greet(row, rem(col + k, D))
        greet(rem(row + k, D), col)

    load.wait()
    at[...] = jnp.transpose(a_ref[...])
    pl.semaphore_wait(barrier, 46)

    def far_first(k):
        return rem(col + 24 + (1 - 2 * rem(k, 2)) * div(k + 1, 2), D)

    if "f" in st:
        piece = T * col
        low = sbuf.at[row, rows(piece, T), :]
        high = sbuf.at[mirror, rows(T * (16 - row) + piece, T), :]

        @pl.when(full)
        def _():
            @pl.loop(0, D)
            def _(k):
                i = far_first(k)
                remote(at.at[rows(T * i, T), pl.ds(H, H)], high, own_send, own_recv.at[16 - row + col], mirror, i).start()

            @pl.loop(0, D - 1)
            def _(k):
                i = far_first(k)
                remote(at.at[rows(T * i, T), pl.ds(0, H)], low, own_send, own_recv.at[col], row, i).start()

            pltpu.make_async_copy(at.at[rows(piece, T), pl.ds(0, H)], low, own_recv.at[col]).start()


    if "x" in st:

        def pass_on(c, place, q, second):
            wait_bytes(sbuf.at[row, rows(T * place, T), :], own_recv.at[place])
            late = div(c, 8)
            start = T * (late * (q - c) + (1 - late) * (16 + c - q)) + Q * second
            dst = jbuf.at[col, rows(start, Q), :]
            for n, r in enumerate((c, 15 - c)):
                src = sbuf.at[row, rows(T * place + Q * n, Q), :]

                @pl.when(r == row)
                def _(src=src):
                    pltpu.make_async_copy(src, dst, x_recv).start()

                @pl.when(r != row)
                def _(src=src, r=r):
                    remote(src, dst, x_send, x_recv, r, col).start()

        @pl.loop(0, D)
        def _(k):
            c = far_first(k)

            @pl.when(c <= mirror)
            def _():
                pass_on(c, row + 1 + c, mirror, 1)

        @pl.loop(0, D)
        def _(k):
            c = far_first(k)

            @pl.when(c <= row)
            def _():
                pass_on(c, c, row, 0)

    s_sent = []

    def s_row(dx, dy, sg):
        return rem(x - sg * dx + 8, 4) * 4 + rem(y - sg * dy + 8, 4)

    def s_copy(h, slot, tx, ty, sg):
        part = sbuf.at[slot, pl.ds(h * half, half), :]
        c = remote(part, part, s_send.at[len(s_sent)], s_recv.at[h, slot], s_row(-tx, -ty, sg), col)
        c.start()
        s_sent.append(c)

    def s_step(d1, d2):
        if "s" not in st:
            return
        for h in range(2):
            sg = sign if h == 0 else -sign
            turn = (lambda p, s: (p, s)) if h == 0 else (lambda p, s: (s, p))
            slot = s_row(*turn(d1, d2), sg)
            if (d1, d2) != (0, 0):
                wait_bytes(sbuf.at[slot, pl.ds(h * half, half), :], s_recv.at[h, slot])
            if d2 == 0:
                if d1 in (0, 1):
                    s_copy(h, slot, *turn(1, 0), sg)
                if d1 == 0:
                    s_copy(h, slot, *turn(-1, 0), sg)
                s_copy(h, slot, *turn(0, 1), sg)
                s_copy(h, slot, *turn(0, -1), sg)
            elif d2 == 1:
                s_copy(h, slot, *turn(0, 1), sg)

    j_sent = []
    other = col + sign

    def z_at(d):
        return rem(col + 2 * sign * d + 32, D)

    def j_pass(t, u, targets, own=False):
        if "j" not in st:
            return
        part = jbuf.at[t, pl.ds(T * CUTS[u], T * (CUTS[u + 1] - CUTS[u])), :]
        if not own:
            wait_bytes(part, j_recv.at[t, u])
        for c in targets:
            cp = remote(part, part, j_send.at[len(j_sent)], j_recv.at[t, u], row, c)
            cp.start()
            j_sent.append(cp)

    def j_step(d, u):
        j_pass(z_at(-d), u, ((z_at(1),) if d < 4 else ()) + (other,))
        if d < 4:
            j_pass(z_at(d), u, ((z_at(-1),) if d < 3 else ()) + (other,))

    s_step(0, 0)
    if "x" in st:
        wait_bytes(jbuf.at[col], x_recv)
    for u in range(SUB):
        j_pass(col, u, (z_at(1), z_at(-1)), True)
    for u in range(SUB):
        j_pass(col, u, (other,), True)
    when = [(5.0, s_step, (1, 0)), (5.1, s_step, (-1, 0)), (8.0, s_step, (0, 1)), (9.5, s_step, (2, 0)),
            (12.5, s_step, (1, 1)), (12.6, s_step, (-1, 1)), (17.0, s_step, (2, 1))]
    for d in range(1, 4):
        for u in range(SUB):
            when.append((4 + 5 * d + 6 / SUB * u, j_step, (d, u)))
    for _, step, args in sorted(when, key=lambda e: e[0]):
        step(*args)
    for d1, d2 in [(0, -1), (0, 2), (1, -1), (-1, -1), (1, 2), (-1, 2), (2, -1), (2, 2)]:
        s_step(d1, d2)

    def j_rest(u):
        for d in range(8):
            j_pass(rem(other + 2 * d, D), u, ())

    def right(start):
        return jbuf[:, rows(start, Q), :].reshape(H, H)

    def times(lhs, rhs):
        return lax.dot_general(lhs, rhs, (((1,), (1,)), ((), ())), preferred_element_type=jnp.float32)

    def add(g, q, start):
        n = T * (q + 1)
        acc[g, 0:n, :] += times(sbuf[q, 0:n, :], right(start)) + times(sbuf[15 - q, R - n : R, :], right(start + Q))

    def send(g):
        if "o" in st:

            @pl.loop(1, D)
            def _(k):
                r = rem(row + k, D)
                remote(acc.at[g, rows(T * r, T), :], got.at[g, row], o_send.at[g], o_recv.at[g], r, col).start()

            pltpu.make_async_copy(acc.at[g, rows(T * row, T), :], got.at[g, row], o_recv.at[g]).start()

    acc[...] = jnp.zeros_like(acc)
    for u in (0, 1):
        j_step(4, u)
    for u in (0, 1):
        j_rest(u)
    if "c" in st:
        for q in reversed(range(8, D)):

            @pl.when(q >= 15 - m)
            def _(q=q):
                add(0, q, T * (q - 15 + m))

    send(0)
    for u in (2, 3):
        j_step(4, u)
    j_rest(2)
    if "c" in st:
        for q in reversed(range(5, D)):

            @pl.when(q >= m + 5)
            def _(q=q):
                add(1, q, T * (16 + m - q))

    j_rest(3)
    if "c" in st:
        for q in reversed(range(12)):

            @pl.when(jnp.logical_and(q >= m, q < m + 5))
            def _(q=q):
                add(1, q, T * (16 + m - q))

    send(1)

    mine = alpha_ref[pl.ds(4 * row + div(col, 4), 1), :]
    mine = pltpu.roll(mine, rem(128 - T * rem(col, 4), 128), 1)
    mine = jnp.transpose(jnp.broadcast_to(mine, (128, 128)))[0:T]

    if "f" in st:

        @pl.when(full)
        def _():
            wait_bytes(at.at[pl.ds(0, T * 15 + T // 2), :], own_send)

    if "x" in st:
        wait_bytes(sbuf.at[row, pl.ds(0, B - Q), :], x_send)
    for c in s_sent + j_sent:
        c.wait_send()
    lane = lax.broadcasted_iota(jnp.int32, (T, 128), 1)
    early = rem(lane, T) < Q
    group = [div(lane, T) == m for m in range(4)]
    for g in range(2):
        if "o" in st:
            wait_bytes(got.at[g], o_recv.at[g])
        for b in range(8) if g else range(8, D):
            for k in range(B // 128):
                start = B * b + 128 * k
                wide = []
                for n in range(2):
                    part = got[g, 15 - b if n else b, :, 128 * (k // 2) : 128 * (k // 2 + 1)]
                    for i in range(4):
                        shift = (Q * i - 64 * (k % 2) + Q * n) % 128
                        moved = pltpu.roll(part, shift, 1) if shift else part
                        total = jnp.where(group[i], moved, total) if i else moved
                    wide.append(total)
                out_ref[:, start : start + 128] = (
                    jnp.where(early, *wide) - mine * alpha_ref[start // 128 : start // 128 + 1, :]
                )
    if "o" in st:
        for g in range(2):
            wait_bytes(acc.at[g, pl.ds(0, B - T), :], o_send.at[g])


def solution(mesh, st="fxsjco"):
    def body(a, alpha):
        B = a.shape[0]
        T, H, R = B // D, B // 2, (B // D) * 17
        dma = pltpu.SemaphoreType.DMA
        return pl.pallas_call(
            functools.partial(kernel, st, B),
            out_shape=jax.ShapeDtypeStruct((T, B * D), jnp.float32),
            in_specs=[pl.BlockSpec(memory_space=pltpu.HBM), pl.BlockSpec(memory_space=pltpu.VMEM)],
            out_specs=pl.BlockSpec(memory_space=pltpu.VMEM),
            scratch_shapes=[
                pltpu.VMEM((B, B), jnp.bfloat16),
                pltpu.VMEM((B, B), jnp.bfloat16),
                pltpu.VMEM((D, R, H), jnp.bfloat16),
                pltpu.VMEM((D, R, H), jnp.bfloat16),
                pltpu.VMEM((2, B, H), jnp.float32),
                pltpu.VMEM((2, D, T, H), jnp.float32),
                dma,
                dma((30,)),
                dma((2, D)),
                dma,
                dma((D + 1,)),
                dma,
                dma,
                dma((15 * SUB,)),
                dma((D, SUB)),
                dma((2,)),
                dma((2,)),
            ],
            compiler_params=pltpu.CompilerParams(
                collective_id=0, has_side_effects=True, vmem_limit_bytes=VM
            ),
        )(a, alpha.reshape(B * D // 128, 128))

    return jax.shard_map(
        body, mesh=mesh, in_specs=(P("row", "col"), P(None)), out_specs=P(("row", "col"), None), check_vma=False
    )
```

```python
import functools

import jax
import jax.numpy as jnp
from jax import lax
from jax.experimental import pallas as pl
from jax.experimental.pallas import tpu as pltpu
from jax.sharding import PartitionSpec as P

MESH = pl.DeviceIdType.MESH
D = 16
REACH = 819.0
CUTS = (0, 8, 14, 17)
SUB = len(CUTS) - 1
VM = 40 * 1024 * 1024


def div(a, b):
    return lax.div(a, jnp.int32(b))


def rem(a, b):
    return lax.rem(a, jnp.int32(b))


def fold(c):
    return c + div(c, 8) * (15 - 2 * c)


def place_of(c):
    return 8 * div(c, 8) + 2 * rem(c, 4) + div(rem(c, 8), 4)


def kernel(
    st,
    B,
    a_hbm,
    alpha_ref,
    out_ref,
    a_ref,
    at,
    sbuf,
    jbuf,
    acc,
    code,
    unit,
    got,
    units,
    ready,
    a_sem,
    s_send,
    s_recv,
    own_send,
    own_recv,
    x_send,
    x_recv,
    j_send,
    j_recv,
    o_send,
    o_recv,
    u_send,
    u_recv,
):
    T, H, R = B // D, B // 2, (B // D) * 17
    Q, half = T // 2, R // 2
    row, col = lax.axis_index("row"), lax.axis_index("col")
    x, y, core = div(row, 4), rem(row, 4), rem(col, 2)
    sign = 1 - 2 * core
    mirror = 15 - row
    full = row >= col
    m = fold(row)

    def rows(start, n):
        return pl.ds(pl.multiple_of(start, Q), n)

    def remote(src, dst, send, recv, r, c):
        return pltpu.make_async_remote_copy(
            src_ref=src, dst_ref=dst, send_sem=send, recv_sem=recv, device_id=(r, c), device_id_type=MESH
        )

    def wait_bytes(ref, sem):
        pltpu.make_async_copy(ref, ref, sem).wait()

    barrier = pltpu.get_barrier_semaphore()

    def greet(r, c):
        pl.semaphore_signal(barrier, inc=1, device_id=(r, c), device_id_type=MESH)

    load = pltpu.make_async_copy(a_hbm, a_ref, a_sem)
    load.start()

    @pl.loop(1, D)
    def _(k):
        greet(row, rem(col + k, D))
        greet(rem(row + k, D), col)

    load.wait()
    at[...] = jnp.transpose(a_ref[...])
    pl.semaphore_wait(barrier, 30)
    pl.semaphore_signal(ready, inc=1, device_id=(mirror, col), device_id_type=MESH)

    def far_first(k):
        return rem(col + 24 + (1 - 2 * rem(k, 2)) * div(k + 1, 2), D)

    if "f" not in st:
        pl.semaphore_wait(ready, 1)
    if "f" in st:
        piece = T * col
        low = sbuf.at[row, rows(piece, T), :]
        high = sbuf.at[mirror, rows(T * (16 - row) + piece, T), :]

        pl.semaphore_wait(ready, 1)

        @pl.when(full)
        def _():
            @pl.loop(0, D)
            def _(k):
                i = far_first(k)
                remote(at.at[rows(T * i, T), pl.ds(H, H)], high, own_send, own_recv.at[16 - row + col], mirror, i).start()

        @pl.when(full)
        def _():
            @pl.loop(0, D - 1)
            def _(k):
                i = far_first(k)
                remote(at.at[rows(T * i, T), pl.ds(0, H)], low, own_send, own_recv.at[col], row, i).start()

            pltpu.make_async_copy(at.at[rows(piece, T), pl.ds(0, H)], low, own_recv.at[col]).start()

    if "x" in st:

        def pass_on(c, place, q, second):
            wait_bytes(sbuf.at[row, rows(T * place, T), :], own_recv.at[place])
            late = div(c, 8)
            unit_at = late * (q - c) + (1 - late) * (16 + c - q)
            start = T * unit_at + Q * second
            arrived = x_recv.at[sum(div(unit_at + 32 - cut, 32) for cut in CUTS[1:-1])]
            dst = jbuf.at[place_of(col), rows(start, Q), :]
            for n, r in enumerate((c, 15 - c)):
                src = sbuf.at[row, rows(T * place + Q * n, Q), :]

                @pl.when(r == row)
                def _(src=src):
                    pltpu.make_async_copy(src, dst, arrived).start()

                @pl.when(r != row)
                def _(src=src, r=r):
                    remote(src, dst, x_send, arrived, r, col).start()

        @pl.loop(0, D)
        def _(k):
            c = far_first(k)

            @pl.when(c <= mirror)
            def _():
                pass_on(c, row + 1 + c, mirror, 1)

        @pl.loop(0, D)
        def _(k):
            c = far_first(k)

            @pl.when(c <= row)
            def _():
                pass_on(c, c, row, 0)

    s_sent = []

    def s_row(dx, dy, sg):
        return rem(x - sg * dx + 8, 4) * 4 + rem(y - sg * dy + 8, 4)

    def s_copy(h, slot, tx, ty, sg):
        part = sbuf.at[slot, pl.ds(h * half, half), :]
        c = remote(part, part, s_send.at[len(s_sent)], s_recv.at[h, slot], s_row(-tx, -ty, sg), col)
        c.start()
        s_sent.append(c)

    def s_step(d1, d2):
        if "s" not in st:
            return
        for h in range(2):
            sg = sign if h == 0 else -sign
            turn = (lambda p, s: (p, s)) if h == 0 else (lambda p, s: (s, p))
            slot = s_row(*turn(d1, d2), sg)
            if (d1, d2) != (0, 0):
                wait_bytes(sbuf.at[slot, pl.ds(h * half, half), :], s_recv.at[h, slot])
            if d2 == 0:
                if d1 in (0, 1):
                    s_copy(h, slot, *turn(1, 0), sg)
                if d1 == 0:
                    s_copy(h, slot, *turn(-1, 0), sg)
                s_copy(h, slot, *turn(0, 1), sg)
                s_copy(h, slot, *turn(0, -1), sg)
            elif d2 == 1:
                s_copy(h, slot, *turn(0, 1), sg)

    j_sent = []
    other = col + sign

    def z_at(d):
        return rem(col + 2 * sign * d + 32, D)

    def group_of(t, u):
        return jbuf.at[place_of(t), pl.ds(T * CUTS[u], T * (CUTS[u + 1] - CUTS[u])), :]

    def j_pass(t, u, targets, own=False):
        if "j" not in st:
            return
        part = group_of(t, u)
        if not own:
            wait_bytes(part, j_recv.at[place_of(t), u])
        for c in targets:
            cp = remote(part, part, j_send.at[len(j_sent)], j_recv.at[place_of(t), u], row, c)
            cp.start()
            j_sent.append(cp)

    def j_step(d, u):
        j_pass(z_at(-d), u, ((z_at(1),) if d < 4 else ()) + (other,))
        if d < 4:
            j_pass(z_at(d), u, ((z_at(-1),) if d < 3 else ()) + (other,))

    s_step(0, 0)
    for u in range(SUB):
        if "x" in st:
            wait_bytes(group_of(col, u), x_recv.at[u])
        j_pass(col, u, (z_at(1), z_at(-1)), True)
    for u in range(SUB):
        j_pass(col, u, (other,), True)
    when = [(5.0, s_step, (1, 0)), (5.1, s_step, (-1, 0)), (8.0, s_step, (0, 1)), (9.5, s_step, (2, 0)),
            (12.5, s_step, (1, 1)), (12.6, s_step, (-1, 1)), (17.0, s_step, (2, 1))]
    for d in range(1, 4):
        for u in range(SUB):
            when.append((4 + 5 * d + 6 / SUB * u, j_step, (d, u)))
    for _, step, args in sorted(when, key=lambda e: e[0]):
        step(*args)
    for d1, d2 in [(0, -1), (0, 2), (1, -1), (-1, -1), (1, 2), (-1, 2), (2, -1), (2, 2)]:
        s_step(d1, d2)

    def j_rest(u):
        for d in range(8):
            j_pass(rem(other + 2 * d, D), u, ())

    def right(start):
        return jbuf[:, rows(start, Q), :].reshape(H, H)

    def times(lhs, rhs):
        return lax.dot_general(lhs, rhs, (((1,), (1,)), ((), ())), preferred_element_type=jnp.float32)

    def add(g, q, start):
        n = T * (q + 1)
        acc[g, 0:n, :] += times(sbuf[q, 0:n, :], right(start)) + times(sbuf[15 - q, R - n : R, :], right(start + Q))

    def send(g):
        if "o" not in st:
            return
        top = jnp.maximum(jnp.max(jnp.abs(acc[g]), keepdims=True), 1e-30)
        one = acc[g] * (REACH / top)
        two = one * one
        four = two * two
        code[g] = (four * four * four * one).astype(jnp.bfloat16)
        unit[g] = jnp.broadcast_to(top * (1.0 / REACH), (8, 128))

        @pl.loop(1, D)
        def _(k):
            r = rem(row + k, D)
            remote(code.at[g, rows(T * r, T), :], got.at[g, row], o_send.at[g], o_recv.at[g], r, col).start()
            remote(unit.at[g], units.at[g, row], u_send.at[g], u_recv.at[g], r, col).start()

        pltpu.make_async_copy(code.at[g, rows(T * row, T), :], got.at[g, row], o_recv.at[g]).start()
        pltpu.make_async_copy(unit.at[g], units.at[g, row], u_recv.at[g]).start()

    acc[...] = jnp.zeros_like(acc)
    light = CUTS.index(8)
    for u in range(light):
        j_step(4, u)
    for u in range(light):
        j_rest(u)
    if "c" in st:
        for q in reversed(range(8, D)):

            @pl.when(q >= 15 - m)
            def _(q=q):
                add(0, q, T * (q - 15 + m))

    send(0)
    high = D
    for u in range(light, SUB):
        j_step(4, u)
    for u in range(light, SUB):
        j_rest(u)
        low = m + 17 - CUTS[u + 1]
        if "c" in st:
            for q in reversed(range(17 - CUTS[u + 1], min(D, 24 - CUTS[u]) if u > light else D)):

                @pl.when(jnp.logical_and(q >= low, q < high))
                def _(q=q):
                    add(1, q, T * (16 + m - q))

        high = low
    send(1)

    mine = alpha_ref[pl.ds(4 * row + div(col, 4), 1), :]
    mine = pltpu.roll(mine, rem(128 - T * rem(col, 4), 128), 1)
    mine = jnp.transpose(jnp.broadcast_to(mine, (128, 128)))[0:T]

    if "f" in st:

        @pl.when(full)
        def _():
            wait_bytes(at.at[pl.ds(0, T * 15 + T // 2), :], own_send)

    if "x" in st:
        wait_bytes(sbuf.at[row, pl.ds(0, B - Q), :], x_send)
    for c in s_sent + j_sent:
        c.wait_send()
    lane = lax.broadcasted_iota(jnp.int32, (T, 128), 1)
    early = rem(lane, T) < Q
    for g in range(2):
        if "o" in st:
            wait_bytes(got.at[g], o_recv.at[g])
            wait_bytes(units.at[g], u_recv.at[g])

        def decode(r, tile, g=g):
            value = got[g, r, :, tile].astype(jnp.float32)
            size = jnp.exp(jnp.log(jnp.abs(value)) * (1.0 / 13.0)) * units[g, r, 0:1, :]
            return jnp.where(value < 0.0, -size, size)

        for b in range(8) if g else range(8, D):
            for k in range(H // 128):
                tile = slice(128 * k, 128 * (k + 1))
                near, far = decode(b, tile), decode(15 - b, tile)
                start = B * b + 256 * k
                for n, value in enumerate(
                    (jnp.where(early, near, pltpu.roll(far, Q, 1)), jnp.where(early, pltpu.roll(near, 128 - Q, 1), far))
                ):
                    first = start + 128 * n
                    out_ref[:, first : first + 128] = value - mine * alpha_ref[first // 128 : first // 128 + 1, :]
    if "o" in st:
        for g in range(2):
            wait_bytes(code.at[g, pl.ds(0, B - T), :], o_send.at[g])
            wait_bytes(units.at[g, pl.ds(0, D - 1)], u_send.at[g])


def solution(mesh, st="fxsjco"):
    def body(a, alpha):
        B = a.shape[0]
        T, H, R = B // D, B // 2, (B // D) * 17
        dma = pltpu.SemaphoreType.DMA
        return pl.pallas_call(
            functools.partial(kernel, st, B),
            out_shape=jax.ShapeDtypeStruct((T, B * D), jnp.float32),
            in_specs=[pl.BlockSpec(memory_space=pltpu.HBM), pl.BlockSpec(memory_space=pltpu.VMEM)],
            out_specs=pl.BlockSpec(memory_space=pltpu.VMEM),
            scratch_shapes=[
                pltpu.VMEM((B, B), jnp.bfloat16),
                pltpu.VMEM((B, B), jnp.bfloat16),
                pltpu.VMEM((D, R, H), jnp.bfloat16),
                pltpu.VMEM((D, R, H), jnp.bfloat16),
                pltpu.VMEM((2, B, H), jnp.float32),
                pltpu.VMEM((2, B, H), jnp.bfloat16),
                pltpu.VMEM((2, 8, 128), jnp.float32),
                pltpu.VMEM((2, D, T, H), jnp.bfloat16),
                pltpu.VMEM((2, D, 8, 128), jnp.float32),
                pltpu.SemaphoreType.REGULAR,
                dma,
                dma((30,)),
                dma((2, D)),
                dma,
                dma((D + 1,)),
                dma,
                dma((SUB,)),
                dma((15 * SUB,)),
                dma((D, SUB)),
                dma((2,)),
                dma((2,)),
                dma((2,)),
                dma((2,)),
            ],
            compiler_params=pltpu.CompilerParams(
                collective_id=0, has_side_effects=True, vmem_limit_bytes=VM
            ),
        )(a, alpha.reshape(B * D // 128, 128))

    return jax.shard_map(
        body, mesh=mesh, in_specs=(P("row", "col"), P(None)), out_specs=P(("row", "col"), None), check_vma=False
    )
```

```python
import functools

import jax
import jax.numpy as jnp
from jax import lax
from jax.experimental import pallas as pl
from jax.experimental.pallas import tpu as pltpu
from jax.sharding import PartitionSpec as P

MESH = pl.DeviceIdType.MESH
D = 16
REACH = 819.0
CUTS = (0, 8, 14, 17)
SUB = len(CUTS) - 1
VM = 40 * 1024 * 1024


def div(a, b):
    return lax.div(a, jnp.int32(b))


def rem(a, b):
    return lax.rem(a, jnp.int32(b))


def fold(c):
    return c + div(c, 8) * (15 - 2 * c)


def place_of(c):
    return 8 * div(c, 8) + 2 * rem(c, 4) + div(rem(c, 8), 4)


def kernel(
    st,
    B,
    a_hbm,
    alpha_ref,
    out_ref,
    a_ref,
    at,
    sbuf,
    jbuf,
    acc,
    code,
    unit,
    got,
    units,
    ready,
    a_sem,
    s_send,
    s_recv,
    own_send,
    own_recv,
    x_send,
    x_recv,
    j_send,
    j_recv,
    o_send,
    o_recv,
    u_send,
    u_recv,
):
    T, H, R = B // D, B // 2, (B // D) * 17
    Q, half = T // 2, R // 2
    row, col = lax.axis_index("row"), lax.axis_index("col")
    x, y, core = div(row, 4), rem(row, 4), rem(col, 2)
    sign = 1 - 2 * core
    mirror = 15 - row
    full = row >= col
    m = fold(row)

    def rows(start, n):
        return pl.ds(pl.multiple_of(start, Q), n)

    def remote(src, dst, send, recv, r, c):
        return pltpu.make_async_remote_copy(
            src_ref=src, dst_ref=dst, send_sem=send, recv_sem=recv, device_id=(r, c), device_id_type=MESH
        )

    def wait_bytes(ref, sem):
        pltpu.make_async_copy(ref, ref, sem).wait()

    barrier = pltpu.get_barrier_semaphore()

    def greet(r, c):
        pl.semaphore_signal(barrier, inc=1, device_id=(r, c), device_id_type=MESH)

    load = pltpu.make_async_copy(a_hbm, a_ref, a_sem)
    load.start()

    @pl.loop(1, D)
    def _(k):
        greet(row, rem(col + k, D))
        greet(rem(row + k, D), col)

    load.wait()
    at[...] = jnp.transpose(a_ref[...])
    pl.semaphore_wait(barrier, 30)
    pl.semaphore_signal(ready, inc=1, device_id=(mirror, col), device_id_type=MESH)

    def far_first(k):
        return rem(col + 24 + (1 - 2 * rem(k, 2)) * div(k + 1, 2), D)

    if "f" not in st:
        pl.semaphore_wait(ready, 1)
    if "f" in st:
        piece = T * col
        low = sbuf.at[row, rows(piece, T), :]
        high = sbuf.at[mirror, rows(T * (16 - row) + piece, T), :]

        pl.semaphore_wait(ready, 1)

        @pl.when(full)
        def _():
            @pl.loop(0, D)
            def _(k):
                i = far_first(k)
                remote(at.at[rows(T * i, T), pl.ds(H, H)], high, own_send, own_recv.at[16 - row + col], mirror, i).start()

        @pl.when(full)
        def _():
            @pl.loop(0, D - 1)
            def _(k):
                i = far_first(k)
                remote(at.at[rows(T * i, T), pl.ds(0, H)], low, own_send, own_recv.at[col], row, i).start()

            pltpu.make_async_copy(at.at[rows(piece, T), pl.ds(0, H)], low, own_recv.at[col]).start()

    if "x" in st:

        def pass_on(c, place, q, second):
            wait_bytes(sbuf.at[row, rows(T * place, T), :], own_recv.at[place])
            late = div(c, 8)
            unit_at = late * (q - c) + (1 - late) * (16 + c - q)
            start = T * unit_at + Q * second
            arrived = x_recv.at[sum(div(unit_at + 32 - cut, 32) for cut in CUTS[1:-1])]
            dst = jbuf.at[place_of(col), rows(start, Q), :]
            for n, r in enumerate((c, 15 - c)):
                src = sbuf.at[row, rows(T * place + Q * n, Q), :]

                @pl.when(r == row)
                def _(src=src):
                    pltpu.make_async_copy(src, dst, arrived).start()

                @pl.when(r != row)
                def _(src=src, r=r):
                    remote(src, dst, x_send, arrived, r, col).start()

        @pl.loop(0, 16 - row)
        def _(c):
            pass_on(c, row + 1 + c, mirror, 1)

        @pl.loop(0, row + 1)
        def _(c):
            pass_on(c, c, row, 0)

    s_sent = []

    def s_row(dx, dy, sg):
        return rem(x - sg * dx + 8, 4) * 4 + rem(y - sg * dy + 8, 4)

    def s_copy(h, slot, tx, ty, sg):
        part = sbuf.at[slot, pl.ds(h * half, half), :]
        c = remote(part, part, s_send.at[len(s_sent)], s_recv.at[h, slot], s_row(-tx, -ty, sg), col)
        c.start()
        s_sent.append(c)

    def s_step(d1, d2):
        if "s" not in st:
            return
        for h in range(2):
            sg = sign if h == 0 else -sign
            turn = (lambda p, s: (p, s)) if h == 0 else (lambda p, s: (s, p))
            slot = s_row(*turn(d1, d2), sg)
            if (d1, d2) != (0, 0):
                wait_bytes(sbuf.at[slot, pl.ds(h * half, half), :], s_recv.at[h, slot])
            if d2 == 0:
                if d1 in (0, 1):
                    s_copy(h, slot, *turn(1, 0), sg)
                if d1 == 0:
                    s_copy(h, slot, *turn(-1, 0), sg)
                s_copy(h, slot, *turn(0, 1), sg)
                s_copy(h, slot, *turn(0, -1), sg)
            elif d2 == 1:
                s_copy(h, slot, *turn(0, 1), sg)

    j_sent = []
    other = col + sign

    def z_at(d):
        return rem(col + 2 * sign * d + 32, D)

    def group_of(t, u):
        return jbuf.at[place_of(t), pl.ds(T * CUTS[u], T * (CUTS[u + 1] - CUTS[u])), :]

    def j_pass(t, u, targets, own=False):
        if "j" not in st:
            return
        part = group_of(t, u)
        if not own:
            wait_bytes(part, j_recv.at[place_of(t), u])
        for c in targets:
            cp = remote(part, part, j_send.at[len(j_sent)], j_recv.at[place_of(t), u], row, c)
            cp.start()
            j_sent.append(cp)

    def j_step(d, u):
        j_pass(z_at(-d), u, ((z_at(1),) if d < 4 else ()) + (other,))
        if d < 4:
            j_pass(z_at(d), u, ((z_at(-1),) if d < 3 else ()) + (other,))

    s_step(0, 0)
    for u in range(SUB):
        if "x" in st:
            wait_bytes(group_of(col, u), x_recv.at[u])
        j_pass(col, u, (z_at(1), z_at(-1)), True)
    for u in range(SUB):
        j_pass(col, u, (other,), True)
    when = [(5.0, s_step, (1, 0)), (5.1, s_step, (-1, 0)), (8.0, s_step, (0, 1)), (9.5, s_step, (2, 0)),
            (12.5, s_step, (1, 1)), (12.6, s_step, (-1, 1)), (17.0, s_step, (2, 1))]
    for d in range(1, 4):
        for u in range(SUB):
            when.append((2 + 5 * d + u, j_step, (d, u)))
    for _, step, args in sorted(when, key=lambda e: e[0]):
        step(*args)
    for d1, d2 in [(0, -1), (0, 2), (1, -1), (-1, -1), (1, 2), (-1, 2), (2, -1), (2, 2)]:
        s_step(d1, d2)

    def j_rest(u):
        for d in range(8):
            j_pass(rem(other + 2 * d, D), u, ())

    def right(start):
        return jbuf[:, rows(start, Q), :].reshape(H, H)

    def times(lhs, rhs):
        return lax.dot_general(lhs, rhs, (((1,), (1,)), ((), ())), preferred_element_type=jnp.float32)

    def add(g, q, start):
        n = T * (q + 1)
        acc[g, 0:n, :] += times(sbuf[q, 0:n, :], right(start)) + times(sbuf[15 - q, R - n : R, :], right(start + Q))

    def send(g):
        if "o" not in st:
            return
        top = jnp.maximum(jnp.max(jnp.abs(acc[g]), keepdims=True), 1e-30)
        one = acc[g] * (REACH / top)
        two = one * one
        four = two * two
        code[g] = (four * four * four * one).astype(jnp.bfloat16)
        unit[g] = jnp.broadcast_to(top * (1.0 / REACH), (8, 128))

        @pl.loop(1, D)
        def _(k):
            r = rem(row + k, D)
            remote(code.at[g, rows(T * r, T), :], got.at[g, row], o_send.at[g], o_recv.at[g], r, col).start()
            remote(unit.at[g], units.at[g, row], u_send.at[g], u_recv.at[g], r, col).start()

        pltpu.make_async_copy(code.at[g, rows(T * row, T), :], got.at[g, row], o_recv.at[g]).start()
        pltpu.make_async_copy(unit.at[g], units.at[g, row], u_recv.at[g]).start()

    acc[...] = jnp.zeros_like(acc)
    light = CUTS.index(8)
    for u in range(light):
        j_step(4, u)
    for u in range(light):
        j_rest(u)
    def sums(g, lo, hi):
        for block in range(8) if "c" in st else ():

            @pl.when(m == block)
            def _(block=block):
                for q in reversed(range(15 - block if g == 0 else block, D)):
                    place = q - 15 + block if g == 0 else 16 + block - q
                    if lo <= place < hi:
                        add(g, q, T * place)

    sums(0, 0, 8)
    send(0)
    for u in range(light, SUB):
        j_step(4, u)
    for u in range(light, SUB):
        j_rest(u)
        sums(1, 0 if u == light else CUTS[u], CUTS[u + 1])
    send(1)

    mine = alpha_ref[pl.ds(4 * row + div(col, 4), 1), :]
    mine = pltpu.roll(mine, rem(128 - T * rem(col, 4), 128), 1)
    mine = jnp.transpose(jnp.broadcast_to(mine, (128, 128)))[0:T]

    if "f" in st:

        @pl.when(full)
        def _():
            wait_bytes(at.at[pl.ds(0, T * 15 + T // 2), :], own_send)

    if "x" in st:
        wait_bytes(sbuf.at[row, pl.ds(0, B - Q), :], x_send)
    for c in s_sent + j_sent:
        c.wait_send()
    lane = lax.broadcasted_iota(jnp.int32, (T, 128), 1)
    early = rem(lane, T) < Q
    for g in range(2):
        if "o" in st:
            wait_bytes(got.at[g], o_recv.at[g])
            wait_bytes(units.at[g], u_recv.at[g])

        def decode(r, tile, g=g):
            value = got[g, r, :, tile].astype(jnp.float32)
            size = jnp.exp(jnp.log(jnp.abs(value)) * (1.0 / 13.0)) * units[g, r, 0:1, :]
            return jnp.where(value < 0.0, -size, size)

        for b in range(8) if g else range(8, D):
            for k in range(H // 128):
                tile = slice(128 * k, 128 * (k + 1))
                near, far = decode(b, tile), decode(15 - b, tile)
                start = B * b + 256 * k
                for n, value in enumerate(
                    (jnp.where(early, near, pltpu.roll(far, Q, 1)), jnp.where(early, pltpu.roll(near, 128 - Q, 1), far))
                ):
                    first = start + 128 * n
                    out_ref[:, first : first + 128] = value - mine * alpha_ref[first // 128 : first // 128 + 1, :]
    if "o" in st:
        for g in range(2):
            wait_bytes(code.at[g, pl.ds(0, B - T), :], o_send.at[g])
            wait_bytes(units.at[g, pl.ds(0, D - 1)], u_send.at[g])


def solution(mesh, st="fxsjco"):
    def body(a, alpha):
        B = a.shape[0]
        T, H, R = B // D, B // 2, (B // D) * 17
        dma = pltpu.SemaphoreType.DMA
        return pl.pallas_call(
            functools.partial(kernel, st, B),
            out_shape=jax.ShapeDtypeStruct((T, B * D), jnp.float32),
            in_specs=[pl.BlockSpec(memory_space=pltpu.HBM), pl.BlockSpec(memory_space=pltpu.VMEM)],
            out_specs=pl.BlockSpec(memory_space=pltpu.VMEM),
            scratch_shapes=[
                pltpu.VMEM((B, B), jnp.bfloat16),
                pltpu.VMEM((B, B), jnp.bfloat16),
                pltpu.VMEM((D, R, H), jnp.bfloat16),
                pltpu.VMEM((D, R, H), jnp.bfloat16),
                pltpu.VMEM((2, B, H), jnp.float32),
                pltpu.VMEM((2, B, H), jnp.bfloat16),
                pltpu.VMEM((2, 8, 128), jnp.float32),
                pltpu.VMEM((2, D, T, H), jnp.bfloat16),
                pltpu.VMEM((2, D, 8, 128), jnp.float32),
                pltpu.SemaphoreType.REGULAR,
                dma,
                dma((30,)),
                dma((2, D)),
                dma,
                dma((D + 1,)),
                dma,
                dma((SUB,)),
                dma((15 * SUB,)),
                dma((D, SUB)),
                dma((2,)),
                dma((2,)),
                dma((2,)),
                dma((2,)),
            ],
            compiler_params=pltpu.CompilerParams(
                collective_id=0, has_side_effects=True, vmem_limit_bytes=VM
            ),
        )(a, alpha.reshape(B * D // 128, 128))

    return jax.shard_map(
        body, mesh=mesh, in_specs=(P("row", "col"), P(None)), out_specs=P(("row", "col"), None), check_vma=False
    )
```

```python
import functools

import jax
import jax.numpy as jnp
from jax import lax
from jax.experimental import pallas as pl
from jax.experimental.pallas import tpu as pltpu
from jax.sharding import PartitionSpec as P

MESH = pl.DeviceIdType.MESH
D = 16
REACH = 819.0
CUTS = (0, 8, 12, 17)
SUB = len(CUTS) - 1
VM = 40 * 1024 * 1024


def div(a, b):
    return lax.div(a, jnp.int32(b))


def rem(a, b):
    return lax.rem(a, jnp.int32(b))


def fold(c):
    return c + div(c, 8) * (15 - 2 * c)


def place_of(c):
    return 8 * div(c, 8) + 2 * rem(c, 4) + div(rem(c, 8), 4)


def kernel(
    B,
    a_ref,
    alpha_ref,
    out_ref,
    at,
    sbuf,
    jbuf,
    acc,
    code,
    unit,
    got,
    units,
    ready,
    s_send,
    s_recv,
    own_send,
    own_recv,
    x_send,
    x_recv,
    j_send,
    j_recv,
    o_send,
    o_recv,
    u_send,
    u_recv,
):
    T, H, R = B // D, B // 2, (B // D) * 17
    Q, half = T // 2, R // 2
    row, col = lax.axis_index("row"), lax.axis_index("col")
    x, y, core = div(row, 4), rem(row, 4), rem(col, 2)
    sign = 1 - 2 * core
    mirror = 15 - row
    full = row >= col
    m = fold(row)

    def rows(start, n):
        return pl.ds(pl.multiple_of(start, Q), n)

    def remote(src, dst, send, recv, r, c):
        return pltpu.make_async_remote_copy(
            src_ref=src, dst_ref=dst, send_sem=send, recv_sem=recv, device_id=(r, c), device_id_type=MESH
        )

    def wait_bytes(ref, sem):
        pltpu.make_async_copy(ref, ref, sem).wait()

    barrier = pltpu.get_barrier_semaphore()

    def greet(r, c):
        pl.semaphore_signal(barrier, inc=1, device_id=(r, c), device_id_type=MESH)

    @pl.loop(1, D)
    def _(k):
        greet(row, rem(col + k, D))
        greet(rem(row + k, D), col)

    at[...] = jnp.transpose(a_ref[...])
    acc[...] = jnp.zeros_like(acc)
    pl.semaphore_wait(barrier, 30)
    pl.semaphore_signal(ready, inc=1, device_id=(mirror, col), device_id_type=MESH)

    def far_first(k):
        return rem(col + 24 + (1 - 2 * rem(k, 2)) * div(k + 1, 2), D)

    piece = T * col
    low = sbuf.at[row, rows(piece, T), :]
    high = sbuf.at[mirror, rows(T * (16 - row) + piece, T), :]

    pl.semaphore_wait(ready, 1)

    @pl.when(full)
    def _():
        @pl.loop(0, D)
        def _(k):
            i = far_first(k)
            remote(at.at[rows(T * i, T), pl.ds(H, H)], high, own_send, own_recv.at[16 - row + col], mirror, i).start()

    @pl.when(full)
    def _():
        @pl.loop(0, D - 1)
        def _(k):
            i = far_first(k)
            remote(at.at[rows(T * i, T), pl.ds(0, H)], low, own_send, own_recv.at[col], row, i).start()

        pltpu.make_async_copy(at.at[rows(piece, T), pl.ds(0, H)], low, own_recv.at[col]).start()


    def pass_on(c, place, q, second):
        wait_bytes(sbuf.at[row, rows(T * place, T), :], own_recv.at[place])
        late = div(c, 8)
        unit_at = late * (q - c) + (1 - late) * (16 + c - q)
        start = T * unit_at + Q * second
        arrived = x_recv.at[sum(div(unit_at + 32 - cut, 32) for cut in CUTS[1:-1])]
        dst = jbuf.at[place_of(col), rows(start, Q), :]
        for n, r in enumerate((c, 15 - c)):
            src = sbuf.at[row, rows(T * place + Q * n, Q), :]

            @pl.when(r == row)
            def _(src=src):
                pltpu.make_async_copy(src, dst, arrived).start()

            @pl.when(r != row)
            def _(src=src, r=r):
                remote(src, dst, x_send, arrived, r, col).start()

    @pl.loop(0, 16 - row)
    def _(c):
        pass_on(c, row + 1 + c, mirror, 1)

    @pl.loop(0, row + 1)
    def _(c):
        pass_on(c, c, row, 0)

    s_sent = []

    def s_row(dx, dy, sg):
        return rem(x - sg * dx + 8, 4) * 4 + rem(y - sg * dy + 8, 4)

    def s_copy(h, slot, tx, ty, sg):
        part = sbuf.at[slot, pl.ds(h * half, half), :]
        c = remote(part, part, s_send.at[len(s_sent)], s_recv.at[h, slot], s_row(-tx, -ty, sg), col)
        c.start()
        s_sent.append(c)

    def s_step(d1, d2):
        for h in range(2):
            sg = sign if h == 0 else -sign
            turn = (lambda p, s: (p, s)) if h == 0 else (lambda p, s: (s, p))
            slot = s_row(*turn(d1, d2), sg)
            if (d1, d2) != (0, 0):
                wait_bytes(sbuf.at[slot, pl.ds(h * half, half), :], s_recv.at[h, slot])
            if d2 == 0:
                if d1 in (0, 1):
                    s_copy(h, slot, *turn(1, 0), sg)
                if d1 == 0:
                    s_copy(h, slot, *turn(-1, 0), sg)
                s_copy(h, slot, *turn(0, 1), sg)
                s_copy(h, slot, *turn(0, -1), sg)
            elif d2 == 1:
                s_copy(h, slot, *turn(0, 1), sg)

    j_sent = []
    other = col + sign

    def z_at(d):
        return rem(col + 2 * sign * d + 32, D)

    def group_of(t, u):
        return jbuf.at[place_of(t), pl.ds(T * CUTS[u], T * (CUTS[u + 1] - CUTS[u])), :]

    def j_pass(t, u, targets, own=False):
        part = group_of(t, u)
        if not own:
            wait_bytes(part, j_recv.at[place_of(t), u])
        for c in targets:
            cp = remote(part, part, j_send.at[len(j_sent)], j_recv.at[place_of(t), u], row, c)
            cp.start()
            j_sent.append(cp)

    def j_step(d, u):
        j_pass(z_at(-d), u, ((z_at(1),) if d < 4 else ()) + (other,))
        if d < 4:
            j_pass(z_at(d), u, ((z_at(-1),) if d < 3 else ()) + (other,))

    s_step(0, 0)
    for u in range(SUB):
        wait_bytes(group_of(col, u), x_recv.at[u])
        j_pass(col, u, (z_at(1), z_at(-1)), True)
    for u in range(SUB):
        j_pass(col, u, (other,), True)
    when = [(5.0, s_step, (1, 0)), (5.1, s_step, (-1, 0)), (8.0, s_step, (0, 1)), (9.5, s_step, (2, 0)),
            (12.5, s_step, (1, 1)), (12.6, s_step, (-1, 1)), (17.0, s_step, (2, 1))]
    for d in range(1, 4):
        for u in range(SUB):
            when.append((2 + 5 * d + u, j_step, (d, u)))
    for _, step, args in sorted(when, key=lambda e: e[0]):
        step(*args)
    for d1, d2 in [(0, -1), (0, 2), (1, -1), (-1, -1), (1, 2), (-1, 2), (2, -1), (2, 2)]:
        s_step(d1, d2)

    def j_rest(u):
        for d in range(8):
            j_pass(rem(other + 2 * d, D), u, ())

    def right(start):
        return jbuf[:, rows(start, Q), :].reshape(H, H)

    def times(lhs, rhs):
        return lax.dot_general(lhs, rhs, (((1,), (1,)), ((), ())), preferred_element_type=jnp.float32)

    def add(g, q, start):
        n = T * (q + 1)
        acc[g, 0:n, :] += times(sbuf[q, 0:n, :], right(start)) + times(sbuf[15 - q, R - n : R, :], right(start + Q))

    def send(g):
        top = jnp.maximum(jnp.max(jnp.abs(acc[g]), keepdims=True), 1e-30)
        one = acc[g] * (REACH / top)
        two = one * one
        four = two * two
        code[g] = (four * four * four * one).astype(jnp.bfloat16)
        unit[g] = jnp.broadcast_to(top * (1.0 / REACH), (8, 128))

        @pl.loop(1, D)
        def _(k):
            r = rem(row + k, D)
            remote(code.at[g, rows(T * r, T), :], got.at[g, row], o_send.at[g], o_recv.at[g], r, col).start()
            remote(unit.at[g], units.at[g, row], u_send.at[g], u_recv.at[g], r, col).start()

        pltpu.make_async_copy(code.at[g, rows(T * row, T), :], got.at[g, row], o_recv.at[g]).start()
        pltpu.make_async_copy(unit.at[g], units.at[g, row], u_recv.at[g]).start()

    light = CUTS.index(8)
    for u in range(light):
        j_step(4, u)
    for u in range(light):
        j_rest(u)
    def sums(g, lo, hi):
        for block in range(8):

            @pl.when(m == block)
            def _(block=block):
                for q in reversed(range(15 - block if g == 0 else block, D)):
                    place = q - 15 + block if g == 0 else 16 + block - q
                    if lo <= place < hi:
                        add(g, q, T * place)

    sums(0, 0, 8)
    send(0)
    for u in range(light, SUB):
        j_step(4, u)
    for u in range(light, SUB):
        j_rest(u)
        sums(1, 0 if u == light else CUTS[u], CUTS[u + 1])
    send(1)

    mine = alpha_ref[pl.ds(4 * row + div(col, 4), 1), :]
    mine = pltpu.roll(mine, rem(128 - T * rem(col, 4), 128), 1)
    mine = jnp.transpose(jnp.broadcast_to(mine, (128, 128)))[0:T]


    @pl.when(full)
    def _():
        wait_bytes(at.at[pl.ds(0, T * 15 + T // 2), :], own_send)

    wait_bytes(sbuf.at[row, pl.ds(0, B - Q), :], x_send)
    for c in s_sent + j_sent:
        c.wait_send()
    lane = lax.broadcasted_iota(jnp.int32, (T, 128), 1)
    early = rem(lane, T) < Q
    for g in range(2):
        wait_bytes(got.at[g], o_recv.at[g])
        wait_bytes(units.at[g], u_recv.at[g])

        def decode(r, tile, g=g):
            value = got[g, r, :, tile].astype(jnp.float32)
            size = jnp.exp2(jnp.log(jnp.abs(value)) * (1.4426950408889634 / 13.0)) * units[g, r, 0:1, :]
            return jnp.where(value < 0.0, -size, size)

        for b in range(8) if g else range(8, D):
            for k in range(H // 128):
                tile = slice(128 * k, 128 * (k + 1))
                near, far = decode(b, tile), decode(15 - b, tile)
                start = B * b + 256 * k
                for n, value in enumerate(
                    (jnp.where(early, near, pltpu.roll(far, Q, 1)), jnp.where(early, pltpu.roll(near, 128 - Q, 1), far))
                ):
                    first = start + 128 * n
                    out_ref[:, first : first + 128] = value - mine * alpha_ref[first // 128 : first // 128 + 1, :]
    for g in range(2):
        wait_bytes(code.at[g, pl.ds(0, B - T), :], o_send.at[g])
        wait_bytes(units.at[g, pl.ds(0, D - 1)], u_send.at[g])


def solution(mesh):
    def body(a, alpha):
        B = a.shape[0]
        T, H, R = B // D, B // 2, (B // D) * 17
        dma = pltpu.SemaphoreType.DMA
        return pl.pallas_call(
            functools.partial(kernel, B),
            out_shape=jax.ShapeDtypeStruct((T, B * D), jnp.float32),
            in_specs=[pl.BlockSpec(memory_space=pltpu.VMEM)] * 2,
            out_specs=pl.BlockSpec(memory_space=pltpu.VMEM),
            scratch_shapes=[
                pltpu.VMEM((B, B), jnp.bfloat16),
                pltpu.VMEM((D, R, H), jnp.bfloat16),
                pltpu.VMEM((D, R, H), jnp.bfloat16),
                pltpu.VMEM((2, B, H), jnp.float32),
                pltpu.VMEM((2, B, H), jnp.bfloat16),
                pltpu.VMEM((2, 8, 128), jnp.float32),
                pltpu.VMEM((2, D, T, H), jnp.bfloat16),
                pltpu.VMEM((2, D, 8, 128), jnp.float32),
                pltpu.SemaphoreType.REGULAR,
                dma((30,)),
                dma((2, D)),
                dma,
                dma((D + 1,)),
                dma,
                dma((SUB,)),
                dma((15 * SUB,)),
                dma((D, SUB)),
                dma((2,)),
                dma((2,)),
                dma((2,)),
                dma((2,)),
            ],
            compiler_params=pltpu.CompilerParams(
                collective_id=0, has_side_effects=True, vmem_limit_bytes=VM
            ),
        )(a, alpha.reshape(B * D // 128, 128))

    return jax.shard_map(
        body, mesh=mesh, in_specs=(P("row", "col"), P(None)), out_specs=P(("row", "col"), None), check_vma=False
    )
```

```python
import functools

import jax
import jax.numpy as jnp
from jax import lax
from jax.experimental import pallas as pl
from jax.experimental.pallas import tpu as pltpu
from jax.sharding import PartitionSpec as P

MESH = pl.DeviceIdType.MESH
D = 16
REACH = 819.0
CUTS = (0, 8, 12, 17)
SUB = len(CUTS) - 1
VM = 40 * 1024 * 1024


def div(a, b):
    return lax.div(a, jnp.int32(b))


def rem(a, b):
    return lax.rem(a, jnp.int32(b))


def fold(c):
    return c + div(c, 8) * (15 - 2 * c)


def place_of(c):
    return 8 * div(c, 8) + 2 * rem(c, 4) + div(rem(c, 8), 4)


def kernel(
    B,
    a_ref,
    alpha_ref,
    out_ref,
    at,
    sbuf,
    jbuf,
    acc,
    code,
    unit,
    got,
    units,
    ready,
    s_send,
    s_recv,
    own_send,
    own_recv,
    x_send,
    x_recv,
    j_send,
    j_recv,
    o_send,
    o_recv,
    u_send,
    u_recv,
):
    T, H, R = B // D, B // 2, (B // D) * 17
    Q, half = T // 2, R // 2
    row, col = lax.axis_index("row"), lax.axis_index("col")
    x, y, core = div(row, 4), rem(row, 4), rem(col, 2)
    sign = 1 - 2 * core
    mirror = 15 - row
    full = row >= col
    m = fold(row)

    def rows(start, n):
        return pl.ds(pl.multiple_of(start, Q), n)

    def remote(src, dst, send, recv, r, c):
        return pltpu.make_async_remote_copy(
            src_ref=src, dst_ref=dst, send_sem=send, recv_sem=recv, device_id=(r, c), device_id_type=MESH
        )

    def wait_bytes(ref, sem):
        pltpu.make_async_copy(ref, ref, sem).wait()

    barrier = pltpu.get_barrier_semaphore()

    def greet(r, c):
        pl.semaphore_signal(barrier, inc=1, device_id=(r, c), device_id_type=MESH)

    @pl.loop(1, D, unroll=True)
    def _(k):
        greet(row, rem(col + k, D))
        greet(rem(row + k, D), col)

    at[...] = jnp.transpose(a_ref[...])
    acc[...] = jnp.zeros_like(acc)
    pl.semaphore_wait(barrier, 30)
    pl.semaphore_signal(ready, inc=1, device_id=(mirror, col), device_id_type=MESH)

    def far_first(k):
        return rem(col + 24 + (1 - 2 * rem(k, 2)) * div(k + 1, 2), D)

    piece = T * col
    low = sbuf.at[row, rows(piece, T), :]
    high = sbuf.at[mirror, rows(T * (16 - row) + piece, T), :]

    pl.semaphore_wait(ready, 1)

    @pl.when(full)
    def _():
        @pl.loop(0, D, unroll=True)
        def _(k):
            i = far_first(k)
            remote(at.at[rows(T * i, T), pl.ds(H, H)], high, own_send, own_recv.at[16 - row + col], mirror, i).start()

    @pl.when(full)
    def _():
        @pl.loop(0, D - 1, unroll=True)
        def _(k):
            i = far_first(k)
            remote(at.at[rows(T * i, T), pl.ds(0, H)], low, own_send, own_recv.at[col], row, i).start()

        pltpu.make_async_copy(at.at[rows(piece, T), pl.ds(0, H)], low, own_recv.at[col]).start()


    def pass_on(c, place, q, second):
        wait_bytes(sbuf.at[row, rows(T * place, T), :], own_recv.at[place])
        late = div(c, 8)
        unit_at = late * (q - c) + (1 - late) * (16 + c - q)
        start = T * unit_at + Q * second
        arrived = x_recv.at[sum(div(unit_at + 32 - cut, 32) for cut in CUTS[1:-1])]
        dst = jbuf.at[place_of(col), rows(start, Q), :]
        for n, r in enumerate((c, 15 - c)):
            src = sbuf.at[row, rows(T * place + Q * n, Q), :]

            @pl.when(r == row)
            def _(src=src):
                pltpu.make_async_copy(src, dst, arrived).start()

            @pl.when(r != row)
            def _(src=src, r=r):
                remote(src, dst, x_send, arrived, r, col).start()

    @pl.loop(0, 16 - row)
    def _(c):
        pass_on(c, row + 1 + c, mirror, 1)

    @pl.loop(0, row + 1)
    def _(c):
        pass_on(c, c, row, 0)

    s_sent = []

    def s_row(dx, dy, sg):
        return rem(x - sg * dx + 8, 4) * 4 + rem(y - sg * dy + 8, 4)

    def s_copy(h, slot, tx, ty, sg):
        part = sbuf.at[slot, pl.ds(h * half, half), :]
        c = remote(part, part, s_send.at[len(s_sent)], s_recv.at[h, slot], s_row(-tx, -ty, sg), col)
        c.start()
        s_sent.append(c)

    def s_step(d1, d2):
        for h in range(2):
            sg = sign if h == 0 else -sign
            turn = (lambda p, s: (p, s)) if h == 0 else (lambda p, s: (s, p))
            slot = s_row(*turn(d1, d2), sg)
            if (d1, d2) != (0, 0):
                wait_bytes(sbuf.at[slot, pl.ds(h * half, half), :], s_recv.at[h, slot])
            if d2 == 0:
                if d1 in (0, 1):
                    s_copy(h, slot, *turn(1, 0), sg)
                if d1 == 0:
                    s_copy(h, slot, *turn(-1, 0), sg)
                s_copy(h, slot, *turn(0, 1), sg)
                s_copy(h, slot, *turn(0, -1), sg)
            elif d2 == 1:
                s_copy(h, slot, *turn(0, 1), sg)

    j_sent = []
    other = col + sign

    def z_at(d):
        return rem(col + 2 * sign * d + 32, D)

    def group_of(t, u):
        return jbuf.at[place_of(t), pl.ds(T * CUTS[u], T * (CUTS[u + 1] - CUTS[u])), :]

    def j_pass(t, u, targets, own=False):
        part = group_of(t, u)
        if not own:
            wait_bytes(part, j_recv.at[place_of(t), u])
        for c in targets:
            cp = remote(part, part, j_send.at[len(j_sent)], j_recv.at[place_of(t), u], row, c)
            cp.start()
            j_sent.append(cp)

    def j_step(d, u):
        j_pass(z_at(-d), u, ((z_at(1),) if d < 4 else ()) + (other,))
        if d < 4:
            j_pass(z_at(d), u, ((z_at(-1),) if d < 3 else ()) + (other,))

    s_step(0, 0)
    for u in range(SUB):
        wait_bytes(group_of(col, u), x_recv.at[u])
        j_pass(col, u, (z_at(1), z_at(-1)), True)
    for u in range(SUB):
        j_pass(col, u, (other,), True)
    when = [(5.0, s_step, (1, 0)), (5.1, s_step, (-1, 0)), (8.0, s_step, (0, 1)), (9.5, s_step, (2, 0)),
            (12.5, s_step, (1, 1)), (12.6, s_step, (-1, 1)), (17.0, s_step, (2, 1))]
    for d in range(1, 4):
        for u in range(SUB):
            when.append((2 + 5 * d + u, j_step, (d, u)))
    for _, step, args in sorted(when, key=lambda e: e[0]):
        step(*args)
    for d1, d2 in [(0, -1), (0, 2), (1, -1), (-1, -1), (1, 2), (-1, 2), (2, -1), (2, 2)]:
        s_step(d1, d2)

    def j_rest(u):
        for d in range(8):
            j_pass(rem(other + 2 * d, D), u, ())

    def right(start):
        return jbuf[:, rows(start, Q), :].reshape(H, H)

    def times(lhs, rhs):
        return lax.dot_general(lhs, rhs, (((1,), (1,)), ((), ())), preferred_element_type=jnp.float32)

    def add(g, q, start):
        n = T * (q + 1)
        acc[g, 0:n, :] += times(sbuf[q, 0:n, :], right(start)) + times(sbuf[15 - q, R - n : R, :], right(start + Q))

    def send(g):
        top = jnp.maximum(jnp.max(jnp.abs(acc[g]), keepdims=True), 1e-30)
        one = acc[g] * (REACH / top)
        two = one * one
        four = two * two
        code[g] = (four * four * four * one).astype(jnp.bfloat16)
        unit[g] = jnp.broadcast_to(top * (1.0 / REACH), (8, 128))

        @pl.loop(1, D, unroll=True)
        def _(k):
            r = rem(row + k, D)
            remote(code.at[g, rows(T * r, T), :], got.at[g, row], o_send.at[g], o_recv.at[g], r, col).start()
            remote(unit.at[g], units.at[g, row], u_send.at[g], u_recv.at[g], r, col).start()

        pltpu.make_async_copy(code.at[g, rows(T * row, T), :], got.at[g, row], o_recv.at[g]).start()
        pltpu.make_async_copy(unit.at[g], units.at[g, row], u_recv.at[g]).start()

    light = CUTS.index(8)
    for u in range(light):
        j_step(4, u)
    for u in range(light):
        j_rest(u)
    def sums(g, lo, hi):
        for block in range(8):

            @pl.when(m == block)
            def _(block=block):
                for q in reversed(range(15 - block if g == 0 else block, D)):
                    place = q - 15 + block if g == 0 else 16 + block - q
                    if lo <= place < hi:
                        add(g, q, T * place)

    sums(0, 0, 8)
    send(0)
    for u in range(light, SUB):
        j_step(4, u)
    for u in range(light, SUB):
        j_rest(u)
        sums(1, 0 if u == light else CUTS[u], CUTS[u + 1])
    send(1)

    mine = alpha_ref[pl.ds(4 * row + div(col, 4), 1), :]
    mine = pltpu.roll(mine, rem(128 - T * rem(col, 4), 128), 1)
    mine = jnp.transpose(jnp.broadcast_to(mine, (128, 128)))[0:T]


    @pl.when(full)
    def _():
        wait_bytes(at.at[pl.ds(0, T * 15 + T // 2), :], own_send)

    wait_bytes(sbuf.at[row, pl.ds(0, B - Q), :], x_send)
    for c in s_sent + j_sent:
        c.wait_send()
    lane = lax.broadcasted_iota(jnp.int32, (T, 128), 1)
    early = rem(lane, T) < Q
    for g in range(2):
        wait_bytes(got.at[g], o_recv.at[g])
        wait_bytes(units.at[g], u_recv.at[g])

        def decode(r, tile, g=g):
            value = got[g, r, :, tile].astype(jnp.float32)
            size = jnp.exp2(jnp.log(jnp.abs(value)) * (1.4426950408889634 / 13.0)) * units[g, r, 0:1, :]
            return jnp.where(value < 0.0, -size, size)

        for b in range(8) if g else range(8, D):
            for k in range(H // 128):
                tile = slice(128 * k, 128 * (k + 1))
                near, far = decode(b, tile), decode(15 - b, tile)
                start = B * b + 256 * k
                for n, value in enumerate(
                    (jnp.where(early, near, pltpu.roll(far, Q, 1)), jnp.where(early, pltpu.roll(near, 128 - Q, 1), far))
                ):
                    first = start + 128 * n
                    out_ref[:, first : first + 128] = value - mine * alpha_ref[first // 128 : first // 128 + 1, :]
    for g in range(2):
        wait_bytes(code.at[g, pl.ds(0, B - T), :], o_send.at[g])
        wait_bytes(units.at[g, pl.ds(0, D - 1)], u_send.at[g])


def solution(mesh):
    def body(a, alpha):
        B = a.shape[0]
        T, H, R = B // D, B // 2, (B // D) * 17
        dma = pltpu.SemaphoreType.DMA
        return pl.pallas_call(
            functools.partial(kernel, B),
            out_shape=jax.ShapeDtypeStruct((T, B * D), jnp.float32),
            in_specs=[pl.BlockSpec(memory_space=pltpu.VMEM)] * 2,
            out_specs=pl.BlockSpec(memory_space=pltpu.VMEM),
            scratch_shapes=[
                pltpu.VMEM((B, B), jnp.bfloat16),
                pltpu.VMEM((D, R, H), jnp.bfloat16),
                pltpu.VMEM((D, R, H), jnp.bfloat16),
                pltpu.VMEM((2, B, H), jnp.float32),
                pltpu.VMEM((2, B, H), jnp.bfloat16),
                pltpu.VMEM((2, 8, 128), jnp.float32),
                pltpu.VMEM((2, D, T, H), jnp.bfloat16),
                pltpu.VMEM((2, D, 8, 128), jnp.float32),
                pltpu.SemaphoreType.REGULAR,
                dma((30,)),
                dma((2, D)),
                dma,
                dma((D + 1,)),
                dma,
                dma((SUB,)),
                dma((15 * SUB,)),
                dma((D, SUB)),
                dma((2,)),
                dma((2,)),
                dma((2,)),
                dma((2,)),
            ],
            compiler_params=pltpu.CompilerParams(
                collective_id=0, has_side_effects=True, vmem_limit_bytes=VM
            ),
        )(a, alpha.reshape(B * D // 128, 128))

    return jax.shard_map(
        body, mesh=mesh, in_specs=(P("row", "col"), P(None)), out_specs=P(("row", "col"), None), check_vma=False
    )
```
